32 devices in a mesh: group: 4 (over y, core), freq: 8 (over z, x).
Axes of the slice: x: 2, y: 2, z: 4, core: 2. Of those that a mesh axis runs over, the one named last changes fastest.
Arguments:
- spectra: bfloat16 [2048, 2, 16], P('freq', None, 'group'), may hold values from -6 to 6
- templates: bfloat16 [2048, 2, 2560], P('freq', None, 'group'), may hold values from -600 to 600
- valid_start: int32 [16], replicated, may hold values from 0 to 2048
Outputs:
- peaks: float32 [2560, 16], P('group')
The draws below stay inside these ranges and needn't reach their ends.
All inputs are finite; a program needn't handle non-finite values.
Results may differ from the reference program's by a relative error of at most 0.0019.
Values may be sent and summed in bfloat16 or wider, within the bound.
A program may use at most 256 MiB of HBM per device.

```python
import math
import jax
import jax.numpy as jnp
from jax import lax

N = 4096
K = 2048
VALID = 2048
SEG = 16
TEMPLATES = 2560


def draw_templates(key, part):
    base_key, row_key, col_key = jax.random.split(jax.random.fold_in(key, 11), 3)
    base = jnp.clip(jax.random.normal(base_key, (K, 2, TEMPLATES), jnp.float32), -6.0, 6.0)
    row_scale = jnp.exp(jax.random.uniform(row_key, (TEMPLATES,), jnp.float32, 0.0, math.log(10.0)))
    col_scale = jnp.exp(jax.random.uniform(col_key, (K,), jnp.float32, 0.0, math.log(10.0)))
    return (base * row_scale[None, None, :] * col_scale[:, None, None]).astype(jnp.bfloat16)


def with_ends(values, own_key, smallest, top_value):
    spot = [jax.random.randint(jax.random.fold_in(own_key, axis), (), 0, length) for axis, length in enumerate(values.shape)]
    widest = values.shape.index(max(values.shape))
    beside = spot[:widest] + [(spot[widest] + 1) % values.shape[widest]] + spot[widest + 1:]
    return values.at[tuple(spot)].set(smallest).at[tuple(beside)].set(top_value)


def steps_of(own_key, extent, cuts, smallest, high):
    factor_of = 1.0
    for position, blocks in cuts:
        heights = jax.random.uniform(jax.random.fold_in(jax.random.fold_in(own_key, 6), position), (blocks,), jnp.float32, smallest / len(cuts), high / len(cuts))
        factor_of = factor_of * jnp.repeat(jnp.exp(heights), extent[position] // blocks).reshape((-1,) + (1,) * (len(extent) - 1 - position))
    return factor_of


def noise(own_key, shape, deviation, most, cuts=(), kind=jnp.bfloat16):
    array = jax.random.normal(own_key, shape, jnp.float32) * deviation
    if len(cuts) > 0:
        array = steps_of(own_key, shape, cuts, -0.22, 0.18) * array
    return jnp.clip(array, min=-most, max=most).astype(kind)


def setup_inputs(seed: int = 0) -> dict:
    seeds = jax.random.split(jax.random.key(seed), 4)
    return {
        "spectra": noise(seeds[0], (K, 2, SEG), 1.0, 6.0, ((0, 8), (2, 4))),
        "templates": draw_templates(jax.random.fold_in(seeds[3], 71), 0),
        "valid_start": with_ends(jax.random.randint(seeds[2], (SEG,), 0, N - VALID + 1), jax.random.fold_in(seeds[2], 1), 0, N - VALID).astype(jnp.int32),
    }


def reference(spectra, templates, valid_start):
    bank = jnp.transpose(templates, (1, 2, 0)).astype(jnp.float32)
    strain_all = jnp.transpose(spectra, (1, 2, 0))
    template_norm = jnp.sum(bank[0] * bank[0] + bank[1] * bank[1], axis=1)
    bins_index = jnp.arange(K, dtype=jnp.int32)
    lag_index = jnp.arange(N, dtype=jnp.int32)
    angle = ((bins_index[:, None] * lag_index[None, :]) % N).astype(jnp.float32) * (2.0 * math.pi / N)
    cosine = jnp.cos(angle)
    sine_part = jnp.sin(angle)
    table = jnp.concatenate([jnp.concatenate([cosine, sine_part], 1), jnp.concatenate([-sine_part, cosine], 1)], 0).astype(jnp.bfloat16)

    def one_segment(segment):
        strain = lax.dynamic_index_in_dim(strain_all, segment, 1, False).astype(jnp.float32)
        cross_re = bank[0] * strain[0][None, :] + bank[1] * strain[1][None, :]
        cross_im = bank[0] * strain[1][None, :] - bank[1] * strain[0][None, :]
        cross = jnp.concatenate([cross_re, cross_im], 1).astype(jnp.bfloat16)
        series = jnp.dot(cross, table, preferred_element_type=jnp.float32)
        power = (series[:, :N] * series[:, :N] + series[:, N:] * series[:, N:]) / template_norm[:, None]
        first = valid_start[segment]
        inside = (lag_index >= first) & (lag_index < first + VALID)
        return jnp.max(jnp.where(inside[None, :], power, jnp.float32(0.0)), axis=1)

    peaks = lax.map(one_segment, jnp.arange(SEG, dtype=jnp.int32))
    return peaks.T
```

```python
import functools
import math

import jax
import jax.numpy as jnp
import numpy as np
from jax import lax
from jax.experimental import pallas as pl
from jax.experimental.pallas import tpu as pltpu
from jax.sharding import PartitionSpec as P

LANES = 128
RADIX = 16
SUB = 8
SCALE = 1.1328125


def rotation(angle, row_axis, col_axis):
    cosine, sine = np.cos(angle), np.sin(angle)
    top = np.stack([cosine, -sine], col_axis)
    bottom = np.stack([sine, cosine], col_axis)
    return np.stack([top, bottom], row_axis)


def tables(bins):
    lags = 2 * bins
    inner = lags // RADIX
    a = np.arange(bins // RADIX)
    tau1 = np.arange(inner)
    angle = 2.0 * math.pi * ((tau1[:, None] * a[None, :]) % inner) / inner
    first = rotation(angle.reshape(inner // SUB, SUB, a.size), 1, 2)
    first = first.reshape(inner // SUB, 2, SUB, 2 * a.size)
    turn = 2.0 * math.pi * tau1.reshape(inner // SUB, SUB, 1) / lags
    turn = np.stack([np.cos(turn), np.sin(turn)], 0)
    b = np.arange(RADIX)
    angle = 2.0 * math.pi * ((b[:, None] * b[None, :]) % RADIX) / RADIX
    second = rotation(angle, 0, 2) * SCALE
    second = second.reshape(2 * RADIX, 2 * RADIX)
    second = np.kron(second, np.eye(SUB))
    return first.astype(np.float32), turn.astype(np.float32), second.astype(jnp.bfloat16)


def kernel(valid, r_ref, d_ref, base_ref, turn_ref, w2_ref, vs_ref, out_ref, work_ref, w1_ref, dexp_ref, y_ref):
    step = pl.program_id(0)
    width = out_ref.shape[2]
    parts, _, depth2, _ = r_ref.shape
    depth = depth2 // 2
    segs = d_ref.shape[3]
    per_tile = LANES // segs
    half = parts * depth
    rows2, cols2 = w2_ref.shape
    groups = y_ref.shape[0]
    inner = groups * SUB

    @pl.when(step == 0)
    def _():
        work_ref[...] = base_ref[...]

        @pl.loop(0, RADIX)
        def _(b):
            w1_ref[b] = work_ref[...].reshape(w1_ref.shape[1:]).astype(jnp.bfloat16)
            top, bottom = work_ref[:, 0], work_ref[:, 1]
            cosine, sine = turn_ref[0], turn_ref[1]
            work_ref[:, 0] = top * cosine - bottom * sine
            work_ref[:, 1] = bottom * cosine + top * sine

        seg_spread = (
            lax.broadcasted_iota(jnp.int32, (segs, LANES), 0)
            == lax.broadcasted_iota(jnp.int32, (segs, LANES), 1) // per_tile
        ).astype(jnp.bfloat16)

        @pl.loop(0, RADIX)
        def _(b):
            piece = d_ref[:, b].reshape(2 * half, segs)
            dexp_ref[b] = jnp.dot(piece, seg_spread, preferred_element_type=jnp.float32)

    lane = lax.broadcasted_iota(jnp.int32, (LANES, width), 1)
    wanted = step * (width // segs) + (lane // LANES) * per_tile + lane % per_tile
    pick = (lax.broadcasted_iota(jnp.int32, (LANES, width), 0) == wanted).astype(jnp.bfloat16)

    def split(x):
        x = x.reshape(parts, 2, depth, x.shape[1])
        return x[:, 0].reshape(half, -1), x[:, 1].reshape(half, -1)

    def first_stage(b, norm):
        bank = jnp.dot(
            r_ref[:, b].reshape(2 * half, LANES), pick, preferred_element_type=jnp.float32
        )
        h0, h1 = split(bank)
        d0, d1 = split(dexp_ref[b])
        d0 = jnp.concatenate([d0] * (width // LANES), 1)
        d1 = jnp.concatenate([d1] * (width // LANES), 1)
        square = h0 * h0 + h1 * h1
        norm = norm + jnp.sum(square.reshape(half // SUB, SUB, width), 0)
        cross = jnp.concatenate([h0 * d0 + h1 * d1, h0 * d1 - h1 * d0], 0).astype(jnp.bfloat16)
        y = jnp.dot(w1_ref[b], cross, preferred_element_type=jnp.float32)
        y_ref[:, b] = y.astype(jnp.bfloat16).reshape(groups, 2 * SUB, width)
        return norm

    norm = lax.fori_loop(
        0, RADIX, first_stage, jnp.zeros((SUB, width), jnp.float32), unroll=2
    )
    offset = lax.broadcasted_iota(jnp.int32, (SUB, width), 0) - vs_ref[...]
    row = lax.broadcasted_iota(jnp.int32, (RADIX, SUB, width), 0) * inner

    def second_stage(g, best):
        z = jnp.dot(
            w2_ref[...], y_ref[g].reshape(cols2, width), preferred_element_type=jnp.float32
        )
        re, im = z[: rows2 // 2], z[rows2 // 2 :]
        power = (re * re + im * im).reshape(RADIX, SUB, width)
        late = row + (offset + g * SUB)[None]
        inside = (late >= 0) & (late < valid)
        return jnp.maximum(best, jnp.max(jnp.where(inside, power, 0.0), 0))

    best = lax.fori_loop(
        0, groups, second_stage, jnp.zeros((SUB, width), jnp.float32), unroll=4
    )
    norm = jnp.sum(norm, 0, keepdims=True) * (SCALE * SCALE)
    out_ref[0] = jnp.max(best, 0, keepdims=True) / norm


def correlate(received, strain, starts, rows):
    parts, _, depth2, _ = received.shape
    segs = strain.shape[3]
    bins = parts * RADIX * depth2 // 2
    base, turn, second = tables(bins)
    per_tile = LANES // segs
    tiles = -(-rows // per_tile)
    width = 2 * LANES if tiles % 2 == 0 else LANES
    steps = tiles * LANES // width
    starts = jnp.tile(jnp.repeat(starts, per_tile), width // LANES)
    starts = jnp.broadcast_to(starts[None, :], (SUB, width))
    groups = 2 * bins // RADIX // SUB
    whole = pl.BlockSpec(memory_space=pltpu.VMEM)
    out = pl.pallas_call(
        functools.partial(kernel, bins),
        grid=(steps,),
        out_shape=jax.ShapeDtypeStruct((steps, 1, width), jnp.float32),
        in_specs=[whole] * 6,
        out_specs=pl.BlockSpec((1, 1, width), lambda i: (i, 0, 0)),
        scratch_shapes=[
            pltpu.VMEM(base.shape, jnp.float32),
            pltpu.VMEM((RADIX, groups * 2 * SUB, 2 * bins // RADIX), jnp.bfloat16),
            pltpu.VMEM((RADIX, parts * depth2, LANES), jnp.float32),
            pltpu.VMEM((groups, RADIX, 2 * SUB, width), jnp.bfloat16),
        ],
        compiler_params=pltpu.CompilerParams(vmem_limit_bytes=50 * 1024 * 1024),
    )(received, strain, jnp.asarray(base), jnp.asarray(turn), jnp.asarray(second), starts)
    out = out.reshape(tiles, segs, per_tile)
    return out.transpose(0, 2, 1).reshape(tiles * per_tile, segs)[:rows]


def join_parts(pieces, depth):
    if depth % SUB == 0:
        return pieces
    parts, _, _, last = pieces.shape
    pieces = pieces.reshape(parts, RADIX, 2, depth, last).transpose(1, 2, 0, 3, 4)
    return pieces.reshape(1, RADIX, 2 * parts * depth, last)


def share(piece, axes):
    count = lax.axis_size(axes)
    return lax.all_to_all(jnp.broadcast_to(piece[None], (count,) + piece.shape), axes, 0, 0, tiled=True)


def on_device(spectra, templates, valid_start):
    parts = lax.axis_size("freq")
    bins_here, _, rows_here = templates.shape
    depth = bins_here // RADIX
    rows = rows_here // parts
    bank = templates.reshape(depth, RADIX, 2, parts, rows).transpose(3, 1, 2, 0, 4)
    strain = share(spectra.reshape(bins_here * 2, -1).T, "group")
    segs = strain.shape[0] * strain.shape[1]
    strain = strain.reshape(segs, depth, RADIX, 2).transpose(2, 3, 1, 0)
    strain = jnp.broadcast_to(strain[None], (parts,) + strain.shape)
    bank = jnp.concatenate([bank, strain], 4)
    bank = jnp.pad(bank, ((0, 0),) * 4 + ((0, LANES - rows - segs),))
    bank = bank.reshape(parts, RADIX, 2 * depth, LANES)
    received = lax.all_to_all(bank, "freq", 0, 0, tiled=True)
    strain = received[..., rows : rows + segs]
    peaks = correlate(join_parts(received, depth), join_parts(strain, depth), valid_start, rows)
    peaks = share(peaks.reshape(1, -1), "freq")
    return peaks.reshape(rows_here, -1)


MESH = pl.DeviceIdType.MESH


def fused_tables(bins):
    base, turn, _ = tables(bins)
    groups, _, _, cols = base.shape
    base = base.reshape(groups, 2, SUB, 2, cols // (2 * SUB), SUB)
    base = base.transpose(0, 1, 2, 4, 3, 5).reshape(groups, 2, SUB, cols)
    b = np.arange(RADIX)
    angle = 2.0 * math.pi * ((b[: RADIX // 2, None] * b[None, :]) % RADIX) / RADIX
    second = rotation(angle, 0, 2) * SCALE
    second = np.kron(second.reshape(RADIX, 2 * RADIX), np.eye(SUB))
    return base, turn, second.astype(jnp.bfloat16)


def block_transpose(rows, size):
    count = len(rows)
    lane = lax.broadcasted_iota(jnp.int32, rows[0].shape, rows[0].ndim - 1) // size
    step = count // 2
    while step:
        low = (lane // step) % 2 == 0
        fresh = list(rows)
        for i in range(count):
            if i & step == 0:
                first, second = rows[i], rows[i + step]
                axis = first.ndim - 1
                fresh[i] = jnp.where(low, first, pltpu.roll(second, size * step, axis))
                fresh[i + step] = jnp.where(low, pltpu.roll(first, LANES - size * step, axis), second)
        rows = fresh
        step //= 2
    return rows


def fused_kernel(
    x_hbm, s_ref, vs_ref, base_hbm, turn_hbm, w2_hbm, out_ref,
    x_ref, send_ref, recv_ref, work_ref, turn_ref, w2_ref, w1_ref, strain_ref, dexp_ref, y_ref, peak_ref,
    load_sem, table_sem, send_sem, recv_sem, ssend_sem, srecv_sem, gsend_sem, grecv_sem, psend_sem, precv_sem,
):
    tiles, parts = recv_ref.shape[:2]
    halves, highs = recv_ref.shape[2:4]
    lows = RADIX // highs
    size = LANES // parts
    segs = vs_ref.shape[0]
    width = y_ref.shape[3]
    groups = y_ref.shape[0]
    crowd = strain_ref.shape[0]
    bins_here = x_ref.shape[1]
    rows = 2 * SUB * RADIX
    lags = 2 * parts * bins_here
    me = lax.axis_index("freq")
    team = lax.axis_index("group")

    def load(tile):
        return pltpu.make_async_copy(
            x_hbm.at[:, :, pl.ds(tile * LANES, LANES)], x_ref.at[tile], load_sem.at[tile]
        )

    table_copies = [
        pltpu.make_async_copy(base_hbm, work_ref, table_sem.at[0]),
        pltpu.make_async_copy(turn_hbm, turn_ref, table_sem.at[1]),
        pltpu.make_async_copy(w2_hbm, w2_ref, table_sem.at[2]),
    ]
    for tile in range(tiles):
        load(tile).start()
    for copy in table_copies:
        copy.start()

    barrier = pltpu.get_barrier_semaphore()
    for hop in range(1, parts):
        pl.semaphore_signal(
            barrier, inc=1, device_id={"freq": lax.rem(me + hop, parts)}, device_id_type=MESH
        )
    for hop in range(1, crowd):
        pl.semaphore_signal(
            barrier, inc=1, device_id={"group": lax.rem(team + hop, crowd)}, device_id_type=MESH
        )
    pl.semaphore_wait(barrier, parts + crowd - 2)

    def strain_copy(source, target):
        return pltpu.make_async_remote_copy(
            src_ref=s_ref, dst_ref=strain_ref.at[team, source],
            send_sem=ssend_sem.at[target], recv_sem=srecv_sem.at[source],
            device_id={"freq": target}, device_id_type=MESH,
        )

    def team_copy(source, target):
        return pltpu.make_async_remote_copy(
            src_ref=strain_ref.at[team], dst_ref=strain_ref.at[source],
            send_sem=gsend_sem.at[target], recv_sem=grecv_sem.at[source],
            device_id={"group": target}, device_id_type=MESH,
        )

    def bank_copy(tile, source, target):
        return pltpu.make_async_remote_copy(
            src_ref=send_ref.at[tile, target], dst_ref=recv_ref.at[tile, source],
            send_sem=send_sem.at[tile, target], recv_sem=recv_sem.at[tile, source],
            device_id={"freq": target}, device_id_type=MESH,
        )

    def peak_copy(source, target):
        return pltpu.make_async_remote_copy(
            src_ref=peak_ref.at[me], dst_ref=peak_ref.at[source],
            send_sem=psend_sem.at[target], recv_sem=precv_sem.at[source],
            device_id={"freq": target}, device_id_type=MESH,
        )

    def others(count, here):
        return [lax.rem(here + hop, count) for hop in range(1, count)]

    for target in others(parts, me):
        strain_copy(me, target).start()
    strain_ref[team, me] = s_ref[...]

    place = lax.broadcasted_iota(jnp.int32, (rows, rows), 0)
    origin = ((place % SUB) * RADIX + place // (2 * SUB)) * 2 + (place // SUB) % 2
    sort = (lax.broadcasted_iota(jnp.int32, (rows, rows), 1) == origin).astype(jnp.bfloat16)

    def prepare(tile):
        load(tile).wait()
        x = x_ref[tile].reshape(halves, rows, LANES)
        x = jnp.stack([jnp.dot(sort, x[h], preferred_element_type=jnp.float32) for h in range(halves)])
        x = x.reshape(halves * highs, lows, 2 * SUB, LANES)
        x = block_transpose([x[:, i] for i in range(lows)], size)
        for p in range(parts):
            send_ref[tile, p] = x[p].astype(jnp.bfloat16).reshape(halves, highs, 2 * SUB, LANES)
        for target in others(parts, me):
            bank_copy(tile, me, target).start()
        recv_ref[tile, me] = send_ref[tile, me]

    for tile in range(tiles):
        prepare(tile)
        if tile == min(1, tiles - 1):
            for source in others(parts, me):
                strain_copy(source, source).wait_recv()
            for target in others(crowd, team):
                team_copy(team, target).start()

    for copy in table_copies:
        copy.wait()

    @pl.loop(0, RADIX)
    def _(b):
        w1_ref[b] = work_ref[...].reshape(w1_ref.shape[1:]).astype(jnp.bfloat16)
        top, bottom = work_ref[:, 0], work_ref[:, 1]
        cosine, sine = turn_ref[0], turn_ref[1]
        work_ref[:, 0] = top * cosine - bottom * sine
        work_ref[:, 1] = bottom * cosine + top * sine

    for source in others(crowd, team):
        team_copy(source, source).wait_recv()

    spread = (
        lax.broadcasted_iota(jnp.int32, (segs, LANES), 0)
        == lax.broadcasted_iota(jnp.int32, (segs, LANES), 1) % segs
    ).astype(jnp.bfloat16)
    for f in range(parts):
        piece = jnp.concatenate([strain_ref[g, f] for g in range(crowd)], 0)
        piece = lax.dot_general(
            piece, spread, (((0,), (0,)), ((), ())), preferred_element_type=jnp.float32
        )
        piece = piece.reshape(halves, RADIX, 2 * SUB, LANES)
        for h in range(halves):
            dexp_ref[:, f * halves + h] = piece[h]

    seg = lax.broadcasted_iota(jnp.int32, (SUB, LANES), 1) % segs
    shift = jnp.zeros((SUB, LANES), jnp.int32)
    for s in range(segs):
        shift = jnp.where(seg == s, vs_ref[s], shift)
    a = lax.broadcasted_iota(jnp.int32, (parts * halves, SUB, LANES), 0) * SUB
    a = a + lax.broadcasted_iota(jnp.int32, (parts * halves, SUB, LANES), 1)
    unit = 2.0 * math.pi / lags
    phase = ((a * shift[None] * RADIX + lags // 2) % lags - lags // 2).astype(jnp.float32) * unit
    step_phase = shift.astype(jnp.float32) * unit
    step_cos, step_sin = jnp.cos(step_phase)[None], jnp.sin(step_phase)[None]

    def rotate(b, carry):
        cosine, sine = carry
        d0, d1 = dexp_ref[b, :, :SUB], dexp_ref[b, :, SUB:]
        dexp_ref[b, :, :SUB] = d0 * cosine - d1 * sine
        dexp_ref[b, :, SUB:] = d0 * sine + d1 * cosine
        return cosine * step_cos - sine * step_sin, cosine * step_sin + sine * step_cos

    lax.fori_loop(0, RADIX, rotate, (jnp.cos(phase), jnp.sin(phase)))

    blocks = parts * halves
    lane_template = lax.broadcasted_iota(jnp.int32, (LANES, width), 1) // segs
    bank_row = lax.broadcasted_iota(jnp.int32, (LANES, width), 0)
    collect = (bank_row % size == lane_template).astype(jnp.float32)

    @pl.loop(0, tiles)
    def _(tile):
        for source in others(parts, me):
            bank_copy(tile, source, source).wait_recv()

        def first_stage(i, norm):
            pick = (bank_row == i * size + lane_template).astype(jnp.bfloat16)
            for high in range(highs):
                b = high * lows + i
                piece = recv_ref[tile, :, :, high].reshape(blocks * 2 * SUB, LANES)
                bank = jnp.dot(piece, pick, preferred_element_type=jnp.float32)
                bank = bank.reshape(blocks, 2 * SUB, width)
                h0, h1 = bank[:, :SUB], bank[:, SUB:]
                d0, d1 = dexp_ref[b, :, :SUB], dexp_ref[b, :, SUB:]
                d0 = jnp.concatenate([d0] * (width // LANES), 2)
                d1 = jnp.concatenate([d1] * (width // LANES), 2)
                cross = jnp.concatenate([h0 * d0 + h1 * d1, h0 * d1 - h1 * d0], 1)
                cross = cross.reshape(blocks * 2 * SUB, width).astype(jnp.bfloat16)
                y = jnp.dot(w1_ref[b], cross, preferred_element_type=jnp.float32)
                y_ref[:, b] = y.astype(jnp.bfloat16).reshape(groups, 2 * SUB, width)
            return norm

        lax.fori_loop(0, lows, first_stage, 0)

        def add_squares(f, total):
            piece = recv_ref[tile, f].astype(jnp.float32).reshape(-1, SUB, LANES)
            return total + jnp.sum(piece * piece, 0)

        norm = lax.fori_loop(0, parts, add_squares, jnp.zeros((SUB, LANES), jnp.float32))
        norm = jnp.dot(norm, collect, precision=lax.Precision.HIGHEST, preferred_element_type=jnp.float32)
        norm = jnp.sum(norm, 0, keepdims=True) * (SCALE * SCALE)

        def second_stage(g, best):
            z = jnp.dot(
                w2_ref[...], y_ref[g].reshape(w2_ref.shape[1], width), preferred_element_type=jnp.float32
            )
            half = z.shape[0] // 2
            re, im = z[:half], z[half:]
            power = (re * re + im * im).reshape(half // SUB, SUB, width)
            return jnp.maximum(best, jnp.max(power, 0))

        best = lax.fori_loop(
            0, groups, second_stage, jnp.zeros((SUB, width), jnp.float32), unroll=4
        )
        peak_ref[me, tile] = jnp.max(best, 0, keepdims=True) / norm

    for target in others(parts, me):
        peak_copy(me, target).start()
    for source in others(parts, me):
        peak_copy(source, source).wait_recv()
    out_ref[...] = peak_ref[...].reshape(out_ref.shape)
    for target in others(parts, me):
        peak_copy(me, target).wait_send()
        strain_copy(me, target).wait_send()
        for tile in range(tiles):
            bank_copy(tile, me, target).wait_send()
    for target in others(crowd, team):
        team_copy(team, target).wait_send()


def fused(spectra, templates, valid_start):
    parts, crowd = lax.axis_size("freq"), lax.axis_size("group")
    bins_here, _, rows_here = templates.shape
    segs_here = spectra.shape[2]
    segs = segs_here * crowd
    bins = bins_here * parts
    tiles = rows_here // LANES
    halves = bins_here // (SUB * RADIX)
    highs = RADIX // parts
    width = LANES // parts * segs
    base, turn, second = fused_tables(bins)
    strain = spectra.reshape(halves, SUB, RADIX, 2, segs_here).transpose(4, 0, 2, 3, 1)
    strain = strain.reshape(segs_here, 2 * bins_here)
    groups = 2 * bins // RADIX // SUB
    anywhere = pl.BlockSpec(memory_space=pl.ANY)
    whole = pl.BlockSpec(memory_space=pltpu.VMEM)
    dma = pltpu.SemaphoreType.DMA
    chunk = (halves, highs, 2 * SUB, LANES)
    out = pl.pallas_call(
        fused_kernel,
        out_shape=jax.ShapeDtypeStruct((parts, tiles, width), jnp.float32),
        in_specs=[anywhere, whole, pl.BlockSpec(memory_space=pltpu.SMEM), anywhere, anywhere, anywhere],
        out_specs=whole,
        scratch_shapes=[
            pltpu.VMEM((tiles, bins_here, 2, LANES), jnp.bfloat16),
            pltpu.VMEM((tiles, parts) + chunk, jnp.bfloat16),
            pltpu.VMEM((tiles, parts) + chunk, jnp.bfloat16),
            pltpu.VMEM(base.shape, jnp.float32),
            pltpu.VMEM(turn.shape, jnp.float32),
            pltpu.VMEM(second.shape, jnp.bfloat16),
            pltpu.VMEM((RADIX, groups * 2 * SUB, 2 * bins // RADIX), jnp.bfloat16),
            pltpu.VMEM((crowd, parts, segs_here, 2 * bins_here), jnp.bfloat16),
            pltpu.VMEM((RADIX, parts * halves, 2 * SUB, LANES), jnp.float32),
            pltpu.VMEM((groups, RADIX, 2 * SUB, width), jnp.bfloat16),
            pltpu.VMEM((parts, tiles, 1, width), jnp.float32),
            dma((tiles,)), dma((3,)),
            dma((tiles, parts)), dma((tiles, parts)),
            dma((parts,)), dma((parts,)),
            dma((crowd,)), dma((crowd,)),
            dma((parts,)), dma((parts,)),
        ],
        compiler_params=pltpu.CompilerParams(
            vmem_limit_bytes=50 * 1024 * 1024, collective_id=0, has_side_effects=True
        ),
    )(templates, strain, valid_start, jnp.asarray(base), jnp.asarray(turn), jnp.asarray(second))
    return out.transpose(1, 0, 2).reshape(rows_here, segs)


def fits(spectra, templates):
    parts = lax.axis_size("freq")
    segs = spectra.shape[2] * lax.axis_size("group")
    bins_here, _, rows_here = templates.shape
    return (
        parts > 1
        and RADIX % parts == 0
        and rows_here % LANES == 0
        and bins_here % (SUB * RADIX) == 0
        and LANES // parts * segs == 2 * LANES
    )


def dispatch(spectra, templates, valid_start):
    if fits(spectra, templates):
        return fused(spectra, templates, valid_start)
    return on_device(spectra, templates, valid_start)


def solution(mesh):
    in_specs = (P("freq", None, "group"), P("freq", None, "group"), P())
    out_specs = P("group", None)
    return jax.shard_map(
        dispatch, mesh=mesh, in_specs=in_specs, out_specs=out_specs, check_vma=False
    )
```

```python
import functools
import math

import jax
import jax.numpy as jnp
import numpy as np
from jax import lax
from jax.experimental import pallas as pl
from jax.experimental.pallas import tpu as pltpu
from jax.sharding import PartitionSpec as P

LANES = 128
RADIX = 16
SUB = 8
SCALE = 1.1328125


def rotation(angle, row_axis, col_axis):
    cosine, sine = np.cos(angle), np.sin(angle)
    top = np.stack([cosine, -sine], col_axis)
    bottom = np.stack([sine, cosine], col_axis)
    return np.stack([top, bottom], row_axis)


def tables(bins):
    lags = 2 * bins
    inner = lags // RADIX
    a = np.arange(bins // RADIX)
    tau1 = np.arange(inner)
    angle = 2.0 * math.pi * ((tau1[:, None] * a[None, :]) % inner) / inner
    first = rotation(angle.reshape(inner // SUB, SUB, a.size), 1, 2)
    first = first.reshape(inner // SUB, 2, SUB, 2 * a.size)
    turn = 2.0 * math.pi * tau1.reshape(inner // SUB, SUB, 1) / lags
    turn = np.stack([np.cos(turn), np.sin(turn)], 0)
    b = np.arange(RADIX)
    angle = 2.0 * math.pi * ((b[:, None] * b[None, :]) % RADIX) / RADIX
    second = rotation(angle, 0, 2) * SCALE
    second = second.reshape(2 * RADIX, 2 * RADIX)
    second = np.kron(second, np.eye(SUB))
    return first.astype(np.float32), turn.astype(np.float32), second.astype(jnp.bfloat16)


def kernel(valid, r_ref, d_ref, base_ref, turn_ref, w2_ref, vs_ref, out_ref, work_ref, w1_ref, dexp_ref, y_ref):
    step = pl.program_id(0)
    width = out_ref.shape[2]
    parts, _, depth2, _ = r_ref.shape
    depth = depth2 // 2
    segs = d_ref.shape[3]
    per_tile = LANES // segs
    half = parts * depth
    rows2, cols2 = w2_ref.shape
    groups = y_ref.shape[0]
    inner = groups * SUB

    @pl.when(step == 0)
    def _():
        work_ref[...] = base_ref[...]

        @pl.loop(0, RADIX)
        def _(b):
            w1_ref[b] = work_ref[...].reshape(w1_ref.shape[1:]).astype(jnp.bfloat16)
            top, bottom = work_ref[:, 0], work_ref[:, 1]
            cosine, sine = turn_ref[0], turn_ref[1]
            work_ref[:, 0] = top * cosine - bottom * sine
            work_ref[:, 1] = bottom * cosine + top * sine

        seg_spread = (
            lax.broadcasted_iota(jnp.int32, (segs, LANES), 0)
            == lax.broadcasted_iota(jnp.int32, (segs, LANES), 1) // per_tile
        ).astype(jnp.bfloat16)

        @pl.loop(0, RADIX)
        def _(b):
            piece = d_ref[:, b].reshape(2 * half, segs)
            dexp_ref[b] = jnp.dot(piece, seg_spread, preferred_element_type=jnp.float32)

    lane = lax.broadcasted_iota(jnp.int32, (LANES, width), 1)
    wanted = step * (width // segs) + (lane // LANES) * per_tile + lane % per_tile
    pick = (lax.broadcasted_iota(jnp.int32, (LANES, width), 0) == wanted).astype(jnp.bfloat16)

    def split(x):
        x = x.reshape(parts, 2, depth, x.shape[1])
        return x[:, 0].reshape(half, -1), x[:, 1].reshape(half, -1)

    def first_stage(b, norm):
        bank = jnp.dot(
            r_ref[:, b].reshape(2 * half, LANES), pick, preferred_element_type=jnp.float32
        )
        h0, h1 = split(bank)
        d0, d1 = split(dexp_ref[b])
        d0 = jnp.concatenate([d0] * (width // LANES), 1)
        d1 = jnp.concatenate([d1] * (width // LANES), 1)
        square = h0 * h0 + h1 * h1
        norm = norm + jnp.sum(square.reshape(half // SUB, SUB, width), 0)
        cross = jnp.concatenate([h0 * d0 + h1 * d1, h0 * d1 - h1 * d0], 0).astype(jnp.bfloat16)
        y = jnp.dot(w1_ref[b], cross, preferred_element_type=jnp.float32)
        y_ref[:, b] = y.astype(jnp.bfloat16).reshape(groups, 2 * SUB, width)
        return norm

    norm = lax.fori_loop(
        0, RADIX, first_stage, jnp.zeros((SUB, width), jnp.float32), unroll=2
    )
    offset = lax.broadcasted_iota(jnp.int32, (SUB, width), 0) - vs_ref[...]
    row = lax.broadcasted_iota(jnp.int32, (RADIX, SUB, width), 0) * inner

    def second_stage(g, best):
        z = jnp.dot(
            w2_ref[...], y_ref[g].reshape(cols2, width), preferred_element_type=jnp.float32
        )
        re, im = z[: rows2 // 2], z[rows2 // 2 :]
        power = (re * re + im * im).reshape(RADIX, SUB, width)
        late = row + (offset + g * SUB)[None]
        inside = (late >= 0) & (late < valid)
        return jnp.maximum(best, jnp.max(jnp.where(inside, power, 0.0), 0))

    best = lax.fori_loop(
        0, groups, second_stage, jnp.zeros((SUB, width), jnp.float32), unroll=4
    )
    norm = jnp.sum(norm, 0, keepdims=True) * (SCALE * SCALE)
    out_ref[0] = jnp.max(best, 0, keepdims=True) / norm


def correlate(received, strain, starts, rows):
    parts, _, depth2, _ = received.shape
    segs = strain.shape[3]
    bins = parts * RADIX * depth2 // 2
    base, turn, second = tables(bins)
    per_tile = LANES // segs
    tiles = -(-rows // per_tile)
    width = 2 * LANES if tiles % 2 == 0 else LANES
    steps = tiles * LANES // width
    starts = jnp.tile(jnp.repeat(starts, per_tile), width // LANES)
    starts = jnp.broadcast_to(starts[None, :], (SUB, width))
    groups = 2 * bins // RADIX // SUB
    whole = pl.BlockSpec(memory_space=pltpu.VMEM)
    out = pl.pallas_call(
        functools.partial(kernel, bins),
        grid=(steps,),
        out_shape=jax.ShapeDtypeStruct((steps, 1, width), jnp.float32),
        in_specs=[whole] * 6,
        out_specs=pl.BlockSpec((1, 1, width), lambda i: (i, 0, 0)),
        scratch_shapes=[
            pltpu.VMEM(base.shape, jnp.float32),
            pltpu.VMEM((RADIX, groups * 2 * SUB, 2 * bins // RADIX), jnp.bfloat16),
            pltpu.VMEM((RADIX, parts * depth2, LANES), jnp.float32),
            pltpu.VMEM((groups, RADIX, 2 * SUB, width), jnp.bfloat16),
        ],
        compiler_params=pltpu.CompilerParams(vmem_limit_bytes=50 * 1024 * 1024),
    )(received, strain, jnp.asarray(base), jnp.asarray(turn), jnp.asarray(second), starts)
    out = out.reshape(tiles, segs, per_tile)
    return out.transpose(0, 2, 1).reshape(tiles * per_tile, segs)[:rows]


def join_parts(pieces, depth):
    if depth % SUB == 0:
        return pieces
    parts, _, _, last = pieces.shape
    pieces = pieces.reshape(parts, RADIX, 2, depth, last).transpose(1, 2, 0, 3, 4)
    return pieces.reshape(1, RADIX, 2 * parts * depth, last)


def share(piece, axes):
    count = lax.axis_size(axes)
    return lax.all_to_all(jnp.broadcast_to(piece[None], (count,) + piece.shape), axes, 0, 0, tiled=True)


def on_device(spectra, templates, valid_start):
    parts = lax.axis_size("freq")
    bins_here, _, rows_here = templates.shape
    depth = bins_here // RADIX
    rows = rows_here // parts
    bank = templates.reshape(depth, RADIX, 2, parts, rows).transpose(3, 1, 2, 0, 4)
    strain = share(spectra.reshape(bins_here * 2, -1).T, "group")
    segs = strain.shape[0] * strain.shape[1]
    strain = strain.reshape(segs, depth, RADIX, 2).transpose(2, 3, 1, 0)
    strain = jnp.broadcast_to(strain[None], (parts,) + strain.shape)
    bank = jnp.concatenate([bank, strain], 4)
    bank = jnp.pad(bank, ((0, 0),) * 4 + ((0, LANES - rows - segs),))
    bank = bank.reshape(parts, RADIX, 2 * depth, LANES)
    received = lax.all_to_all(bank, "freq", 0, 0, tiled=True)
    strain = received[..., rows : rows + segs]
    peaks = correlate(join_parts(received, depth), join_parts(strain, depth), valid_start, rows)
    peaks = share(peaks.reshape(1, -1), "freq")
    return peaks.reshape(rows_here, -1)


MESH = pl.DeviceIdType.MESH


def fused_tables(bins):
    base, turn, _ = tables(bins)
    groups, _, _, cols = base.shape
    base = base.reshape(groups, 2, SUB, 2, cols // (2 * SUB), SUB)
    base = base.transpose(0, 1, 2, 4, 3, 5).reshape(groups, 2, SUB, cols)
    b = np.arange(RADIX)
    angle = 2.0 * math.pi * ((b[: RADIX * 3 // 4, None] * b[None, :]) % RADIX) / RADIX
    second = rotation(angle, 0, 2) * SCALE
    second = np.kron(second.reshape(-1, 2 * RADIX), np.eye(SUB))
    return base, turn, second.astype(jnp.bfloat16)


def block_transpose(rows, size):
    count = len(rows)
    lane = lax.broadcasted_iota(jnp.int32, rows[0].shape, rows[0].ndim - 1) // size
    step = count // 2
    while step:
        low = (lane // step) % 2 == 0
        fresh = list(rows)
        for i in range(count):
            if i & step == 0:
                first, second = rows[i], rows[i + step]
                axis = first.ndim - 1
                fresh[i] = jnp.where(low, first, pltpu.roll(second, size * step, axis))
                fresh[i + step] = jnp.where(low, pltpu.roll(first, LANES - size * step, axis), second)
        rows = fresh
        step //= 2
    return rows


def fused_kernel(
    x_hbm, s_hbm, vs_ref, base_hbm, turn_hbm, w2_hbm, out_ref,
    x_ref, own_ref, send_ref, recv_ref, work_ref, turn_ref, w2_ref, w1_ref, s_ref, strain_ref, dexp_ref,
    cross_ref, y_ref, peak_ref,
    load_sem, table_sem, send_sem, recv_sem, ssend_sem, srecv_sem, gsend_sem, grecv_sem, psend_sem, precv_sem,
):
    tiles, parts = recv_ref.shape[:2]
    halves, highs = recv_ref.shape[2:4]
    lows = RADIX // highs
    size = LANES // parts
    segs = vs_ref.shape[0]
    width = y_ref.shape[3]
    groups = y_ref.shape[0]
    crowd = strain_ref.shape[0]
    bins_here = x_ref.shape[1]
    rows = 2 * SUB * RADIX
    lags = 2 * parts * bins_here
    inner = lags // RADIX
    quarter = lags // 4
    blocks = parts * halves
    me = lax.axis_index("freq")
    team = lax.axis_index("group")

    def others(count, here):
        return [lax.rem(here + hop, count) for hop in range(1, count)]

    def load(tile):
        return pltpu.make_async_copy(
            x_hbm.at[:, :, pl.ds(tile * LANES, LANES)], x_ref.at[tile], load_sem.at[tile]
        )

    table_copies = [
        pltpu.make_async_copy(s_hbm, own_ref, table_sem.at[0]),
        pltpu.make_async_copy(base_hbm, work_ref, table_sem.at[1]),
        pltpu.make_async_copy(turn_hbm, turn_ref, table_sem.at[2]),
        pltpu.make_async_copy(w2_hbm, w2_ref, table_sem.at[3]),
    ]
    table_copies[0].start()
    for tile in range(tiles):
        load(tile).start()
    for copy in table_copies[1:]:
        copy.start()

    barrier = pltpu.get_barrier_semaphore()
    for target in others(parts, me):
        pl.semaphore_signal(barrier, inc=1, device_id={"freq": target}, device_id_type=MESH)
    for target in others(crowd, team):
        pl.semaphore_signal(barrier, inc=1, device_id={"group": target}, device_id_type=MESH)

    def strain_copy(source, target):
        return pltpu.make_async_remote_copy(
            src_ref=s_ref, dst_ref=strain_ref.at[team, source],
            send_sem=ssend_sem.at[target], recv_sem=srecv_sem.at[source],
            device_id={"freq": target}, device_id_type=MESH,
        )

    def team_copy(source, target):
        return pltpu.make_async_remote_copy(
            src_ref=strain_ref.at[team], dst_ref=strain_ref.at[source],
            send_sem=gsend_sem.at[target], recv_sem=grecv_sem.at[source],
            device_id={"group": target}, device_id_type=MESH,
        )

    def bank_copy(tile, source, target):
        return pltpu.make_async_remote_copy(
            src_ref=send_ref.at[tile, target], dst_ref=recv_ref.at[tile, source],
            send_sem=send_sem.at[tile, target], recv_sem=recv_sem.at[tile, source],
            device_id={"freq": target}, device_id_type=MESH,
        )

    def peak_copy(source, target):
        return pltpu.make_async_remote_copy(
            src_ref=peak_ref.at[me], dst_ref=peak_ref.at[source],
            send_sem=psend_sem.at[target], recv_sem=precv_sem.at[source],
            device_id={"freq": target}, device_id_type=MESH,
        )

    place = lax.broadcasted_iota(jnp.int32, (rows, rows), 0)
    origin = ((place % SUB) * RADIX + place // (2 * SUB)) * 2 + (place // SUB) % 2
    sort = (lax.broadcasted_iota(jnp.int32, (rows, rows), 1) == origin).astype(jnp.bfloat16)

    table_copies[0].wait()
    for tile in range(tiles):
        load(tile).wait()
    strain = own_ref[...].reshape(halves, rows, own_ref.shape[2])
    strain = [
        lax.dot_general(strain[h], sort, (((0,), (1,)), ((), ())), preferred_element_type=jnp.float32)
        for h in range(halves)
    ]
    s_ref[...] = jnp.concatenate(strain, 1).astype(jnp.bfloat16)
    for tile in range(tiles):
        x = x_ref[tile].reshape(halves, rows, LANES)
        x = jnp.stack([jnp.dot(sort, x[h], preferred_element_type=jnp.float32) for h in range(halves)])
        x = x.reshape(halves * highs, lows, 2 * SUB, LANES)
        x = block_transpose([x[:, i] for i in range(lows)], size)
        for p in range(parts):
            send_ref[tile, p] = x[p].astype(jnp.bfloat16).reshape(halves, highs, 2 * SUB, LANES)

    pl.semaphore_wait(barrier, parts + crowd - 2)
    for target in others(parts, me):
        strain_copy(me, target).start()
    for tile in range(tiles):
        for target in others(parts, me):
            bank_copy(tile, me, target).start()
    strain_ref[team, me] = s_ref[...]
    for tile in range(tiles):
        recv_ref[tile, me] = send_ref[tile, me]

    for copy in table_copies[1:]:
        copy.wait()

    @pl.loop(0, RADIX)
    def _(b):
        w1_ref[b] = work_ref[...].reshape(w1_ref.shape[1:]).astype(jnp.bfloat16)
        top, bottom = work_ref[:, 0], work_ref[:, 1]
        cosine, sine = turn_ref[0], turn_ref[1]
        work_ref[:, 0] = top * cosine - bottom * sine
        work_ref[:, 1] = bottom * cosine + top * sine

    for source in others(parts, me):
        strain_copy(source, source).wait_recv()
    for target in others(crowd, team):
        team_copy(team, target).start()
    for source in others(crowd, team):
        team_copy(source, source).wait_recv()

    seg = lax.broadcasted_iota(jnp.int32, (SUB, LANES), 1) % segs
    start = jnp.zeros((SUB, LANES), jnp.int32)
    for s in range(segs):
        start = jnp.where(seg == s, vs_ref[s], start)
    turns = (start >= quarter).astype(jnp.int32) + (start >= 2 * quarter).astype(jnp.int32)
    rest = start - turns * quarter
    step_cos = 1.0 - turns.astype(jnp.float32)
    step_sin = (turns == 1).astype(jnp.float32)

    spread = (
        lax.broadcasted_iota(jnp.int32, (segs, LANES), 0)
        == lax.broadcasted_iota(jnp.int32, (segs, LANES), 1) % segs
    ).astype(jnp.bfloat16)
    unit = (jnp.ones((SUB, LANES), jnp.float32), jnp.zeros((SUB, LANES), jnp.float32))
    factors = [unit]
    for b in range(1, 4):
        c, s = factors[-1]
        factors.append((c * step_cos - s * step_sin, c * step_sin + s * step_cos))
    for f in range(parts):
        piece = jnp.concatenate([strain_ref[g, f] for g in range(crowd)], 0)
        piece = lax.dot_general(
            piece, spread, (((0,), (0,)), ((), ())), preferred_element_type=jnp.float32
        )
        piece = piece.reshape(halves, RADIX, 2, SUB, LANES)
        for h in range(halves):
            for b in range(RADIX):
                c, s = factors[b % 4]
                d0, d1 = piece[h, b, 0], piece[h, b, 1]
                dexp_ref[b, f * halves + h, :SUB] = d0 * c - d1 * s
                dexp_ref[b, f * halves + h, SUB:] = d0 * s + d1 * c

    lane_template = lax.broadcasted_iota(jnp.int32, (LANES, width), 1) // segs
    bank_row = lax.broadcasted_iota(jnp.int32, (LANES, width), 0)
    collect = (bank_row % size == lane_template).astype(jnp.float32)
    offset = lax.broadcasted_iota(jnp.int32, (SUB, LANES), 0) - rest
    offset = jnp.concatenate([offset] * (width // LANES), 1)

    def expand(tile, i):
        pick = (bank_row == i * size + lane_template).astype(jnp.bfloat16)
        for high in range(highs):
            b = high * lows + i
            piece = recv_ref[tile, :, :, high].reshape(blocks * 2 * SUB, LANES)
            bank = jnp.dot(piece, pick, preferred_element_type=jnp.float32)
            bank = bank.reshape(blocks, 2 * SUB, width)
            h0, h1 = bank[:, :SUB], bank[:, SUB:]
            d0, d1 = dexp_ref[b, :, :SUB], dexp_ref[b, :, SUB:]
            d0 = jnp.concatenate([d0] * (width // LANES), 2)
            d1 = jnp.concatenate([d1] * (width // LANES), 2)
            cross = jnp.concatenate([h0 * d0 + h1 * d1, h0 * d1 - h1 * d0], 1)
            cross_ref[b] = cross.reshape(blocks * 2 * SUB, width).astype(jnp.bfloat16)

    def transform(i):
        for high in range(highs):
            b = high * lows + i
            y = jnp.dot(w1_ref[b], cross_ref[b], preferred_element_type=jnp.float32)
            y_ref[:, b] = y.astype(jnp.bfloat16).reshape(groups, 2 * SUB, width)

    def arrive(tile):
        for source in others(parts, me):
            bank_copy(tile, source, source).wait_recv()

    chunk = 4
    arrive(0)
    for i in range(chunk):
        expand(0, i)

    @pl.loop(0, tiles)
    def _(tile):
        @pl.loop(0, lows // chunk - 1)
        def _(step):
            for i in range(chunk):
                transform(step * chunk + i)
                expand(tile, (step + 1) * chunk + i)

        @pl.when(tile + 1 < tiles)
        def _():
            arrive(tile + 1)

        following = jnp.minimum(tile + 1, tiles - 1)
        for i in range(chunk):
            transform(lows - chunk + i)
            expand(following, i)

        def add_squares(f, total):
            piece = recv_ref[tile, f].astype(jnp.float32).reshape(-1, SUB, LANES)
            return total + jnp.sum(piece * piece, 0)

        norm = jnp.zeros((SUB, LANES), jnp.float32)
        for f in range(parts):
            norm = add_squares(f, norm)
        norm = jnp.dot(norm, collect, precision=lax.Precision.HIGHEST, preferred_element_type=jnp.float32)
        norm = jnp.sum(norm, 0, keepdims=True) * (SCALE * SCALE)

        def second_stage(g, best):
            z = jnp.dot(
                w2_ref[...], y_ref[g].reshape(w2_ref.shape[1], width), preferred_element_type=jnp.float32
            )
            z = z.reshape(2, -1, SUB, width)
            for t in range(RADIX // 2):
                re, im = z[0, t], z[1, t]
                if t + RADIX // 2 < z.shape[1]:
                    inside = offset >= -(g * SUB + t * inner)
                    re = jnp.where(inside, re, z[0, t + RADIX // 2])
                    im = jnp.where(inside, im, z[1, t + RADIX // 2])
                best = jnp.maximum(best, re * re + im * im)
            return best

        best = lax.fori_loop(
            0, groups, second_stage, jnp.zeros((SUB, width), jnp.float32), unroll=32
        )
        peak_ref[me, tile] = jnp.max(best, 0, keepdims=True) / norm

    for target in others(parts, me):
        peak_copy(me, target).start()
    for source in others(parts, me):
        peak_copy(source, source).wait_recv()
    out_ref[...] = peak_ref[...].reshape(out_ref.shape)
    for target in others(parts, me):
        peak_copy(me, target).wait_send()
        strain_copy(me, target).wait_send()
        for tile in range(tiles):
            bank_copy(tile, me, target).wait_send()
    for target in others(crowd, team):
        team_copy(team, target).wait_send()


def fused(spectra, templates, valid_start):
    parts, crowd = lax.axis_size("freq"), lax.axis_size("group")
    bins_here, _, rows_here = templates.shape
    segs_here = spectra.shape[2]
    segs = segs_here * crowd
    bins = bins_here * parts
    tiles = rows_here // LANES
    halves = bins_here // (SUB * RADIX)
    highs = RADIX // parts
    width = LANES // parts * segs
    base, turn, second = fused_tables(bins)
    groups = 2 * bins // RADIX // SUB
    far = pl.BlockSpec(memory_space=pltpu.HBM)
    whole = pl.BlockSpec(memory_space=pltpu.VMEM)
    dma = pltpu.SemaphoreType.DMA
    chunk = (halves, highs, 2 * SUB, LANES)
    out = pl.pallas_call(
        fused_kernel,
        out_shape=jax.ShapeDtypeStruct((parts, tiles, width), jnp.float32),
        in_specs=[far, far, pl.BlockSpec(memory_space=pltpu.SMEM), far, far, far],
        out_specs=whole,
        scratch_shapes=[
            pltpu.VMEM((tiles, bins_here, 2, LANES), jnp.bfloat16),
            pltpu.VMEM((bins_here, 2, segs_here), jnp.bfloat16),
            pltpu.VMEM((tiles, parts) + chunk, jnp.bfloat16),
            pltpu.VMEM((tiles, parts) + chunk, jnp.bfloat16),
            pltpu.VMEM(base.shape, jnp.float32),
            pltpu.VMEM(turn.shape, jnp.float32),
            pltpu.VMEM(second.shape, jnp.bfloat16),
            pltpu.VMEM((RADIX, groups * 2 * SUB, 2 * bins // RADIX), jnp.bfloat16),
            pltpu.VMEM((segs_here, 2 * bins_here), jnp.bfloat16),
            pltpu.VMEM((crowd, parts, segs_here, 2 * bins_here), jnp.bfloat16),
            pltpu.VMEM((RADIX, parts * halves, 2 * SUB, LANES), jnp.float32),
            pltpu.VMEM((RADIX, 2 * bins // RADIX, width), jnp.bfloat16),
            pltpu.VMEM((groups, RADIX, 2 * SUB, width), jnp.bfloat16),
            pltpu.VMEM((parts, tiles, 1, width), jnp.float32),
            dma((tiles,)), dma((4,)),
            dma((tiles, parts)), dma((tiles, parts)),
            dma((parts,)), dma((parts,)),
            dma((crowd,)), dma((crowd,)),
            dma((parts,)), dma((parts,)),
        ],
        compiler_params=pltpu.CompilerParams(
            vmem_limit_bytes=60 * 1024 * 1024, collective_id=0, has_side_effects=True
        ),
    )(templates, spectra, valid_start, jnp.asarray(base), jnp.asarray(turn), jnp.asarray(second))
    return out.transpose(1, 0, 2).reshape(rows_here, segs)


def fits(spectra, templates):
    parts = lax.axis_size("freq")
    segs = spectra.shape[2] * lax.axis_size("group")
    bins_here, _, rows_here = templates.shape
    return (
        parts > 1
        and RADIX % parts == 0
        and rows_here % LANES == 0
        and bins_here % (SUB * RADIX) == 0
        and LANES // parts * segs == 2 * LANES
    )


def dispatch(spectra, templates, valid_start):
    if fits(spectra, templates):
        return fused(spectra, templates, valid_start)
    return on_device(spectra, templates, valid_start)


def solution(mesh):
    in_specs = (P("freq", None, "group"), P("freq", None, "group"), P())
    out_specs = P("group", None)
    return jax.shard_map(
        dispatch, mesh=mesh, in_specs=in_specs, out_specs=out_specs, check_vma=False
    )
```

```python
import functools
import math

import jax
import jax.numpy as jnp
import numpy as np
from jax import lax
from jax.experimental import pallas as pl
from jax.experimental.pallas import tpu as pltpu
from jax.sharding import PartitionSpec as P

LANES = 128
RADIX = 16
SUB = 8
SCALE = 1.1328125


def rotation(angle, row_axis, col_axis):
    cosine, sine = np.cos(angle), np.sin(angle)
    top = np.stack([cosine, -sine], col_axis)
    bottom = np.stack([sine, cosine], col_axis)
    return np.stack([top, bottom], row_axis)


def tables(bins):
    lags = 2 * bins
    inner = lags // RADIX
    a = np.arange(bins // RADIX)
    tau1 = np.arange(inner)
    angle = 2.0 * math.pi * ((tau1[:, None] * a[None, :]) % inner) / inner
    first = rotation(angle.reshape(inner // SUB, SUB, a.size), 1, 2)
    first = first.reshape(inner // SUB, 2, SUB, 2 * a.size)
    turn = 2.0 * math.pi * tau1.reshape(inner // SUB, SUB, 1) / lags
    turn = np.stack([np.cos(turn), np.sin(turn)], 0)
    b = np.arange(RADIX)
    angle = 2.0 * math.pi * ((b[:, None] * b[None, :]) % RADIX) / RADIX
    second = rotation(angle, 0, 2) * SCALE
    second = second.reshape(2 * RADIX, 2 * RADIX)
    second = np.kron(second, np.eye(SUB))
    return first.astype(np.float32), turn.astype(np.float32), second.astype(jnp.bfloat16)


def kernel(valid, r_ref, d_ref, base_ref, turn_ref, w2_ref, vs_ref, out_ref, work_ref, w1_ref, dexp_ref, y_ref):
    step = pl.program_id(0)
    width = out_ref.shape[2]
    parts, _, depth2, _ = r_ref.shape
    depth = depth2 // 2
    segs = d_ref.shape[3]
    per_tile = LANES // segs
    half = parts * depth
    rows2, cols2 = w2_ref.shape
    groups = y_ref.shape[0]
    inner = groups * SUB

    @pl.when(step == 0)
    def _():
        work_ref[...] = base_ref[...]

        @pl.loop(0, RADIX)
        def _(b):
            w1_ref[b] = work_ref[...].reshape(w1_ref.shape[1:]).astype(jnp.bfloat16)
            top, bottom = work_ref[:, 0], work_ref[:, 1]
            cosine, sine = turn_ref[0], turn_ref[1]
            work_ref[:, 0] = top * cosine - bottom * sine
            work_ref[:, 1] = bottom * cosine + top * sine

        seg_spread = (
            lax.broadcasted_iota(jnp.int32, (segs, LANES), 0)
            == lax.broadcasted_iota(jnp.int32, (segs, LANES), 1) // per_tile
        ).astype(jnp.bfloat16)

        @pl.loop(0, RADIX)
        def _(b):
            piece = d_ref[:, b].reshape(2 * half, segs)
            dexp_ref[b] = jnp.dot(piece, seg_spread, preferred_element_type=jnp.float32)

    lane = lax.broadcasted_iota(jnp.int32, (LANES, width), 1)
    wanted = step * (width // segs) + (lane // LANES) * per_tile + lane % per_tile
    pick = (lax.broadcasted_iota(jnp.int32, (LANES, width), 0) == wanted).astype(jnp.bfloat16)

    def split(x):
        x = x.reshape(parts, 2, depth, x.shape[1])
        return x[:, 0].reshape(half, -1), x[:, 1].reshape(half, -1)

    def first_stage(b, norm):
        bank = jnp.dot(
            r_ref[:, b].reshape(2 * half, LANES), pick, preferred_element_type=jnp.float32
        )
        h0, h1 = split(bank)
        d0, d1 = split(dexp_ref[b])
        d0 = jnp.concatenate([d0] * (width // LANES), 1)
        d1 = jnp.concatenate([d1] * (width // LANES), 1)
        square = h0 * h0 + h1 * h1
        norm = norm + jnp.sum(square.reshape(half // SUB, SUB, width), 0)
        cross = jnp.concatenate([h0 * d0 + h1 * d1, h0 * d1 - h1 * d0], 0).astype(jnp.bfloat16)
        y = jnp.dot(w1_ref[b], cross, preferred_element_type=jnp.float32)
        y_ref[:, b] = y.astype(jnp.bfloat16).reshape(groups, 2 * SUB, width)
        return norm

    norm = lax.fori_loop(
        0, RADIX, first_stage, jnp.zeros((SUB, width), jnp.float32), unroll=2
    )
    offset = lax.broadcasted_iota(jnp.int32, (SUB, width), 0) - vs_ref[...]
    row = lax.broadcasted_iota(jnp.int32, (RADIX, SUB, width), 0) * inner

    def second_stage(g, best):
        z = jnp.dot(
            w2_ref[...], y_ref[g].reshape(cols2, width), preferred_element_type=jnp.float32
        )
        re, im = z[: rows2 // 2], z[rows2 // 2 :]
        power = (re * re + im * im).reshape(RADIX, SUB, width)
        late = row + (offset + g * SUB)[None]
        inside = (late >= 0) & (late < valid)
        return jnp.maximum(best, jnp.max(jnp.where(inside, power, 0.0), 0))

    best = lax.fori_loop(
        0, groups, second_stage, jnp.zeros((SUB, width), jnp.float32), unroll=4
    )
    norm = jnp.sum(norm, 0, keepdims=True) * (SCALE * SCALE)
    out_ref[0] = jnp.max(best, 0, keepdims=True) / norm


def correlate(received, strain, starts, rows):
    parts, _, depth2, _ = received.shape
    segs = strain.shape[3]
    bins = parts * RADIX * depth2 // 2
    base, turn, second = tables(bins)
    per_tile = LANES // segs
    tiles = -(-rows // per_tile)
    width = 2 * LANES if tiles % 2 == 0 else LANES
    steps = tiles * LANES // width
    starts = jnp.tile(jnp.repeat(starts, per_tile), width // LANES)
    starts = jnp.broadcast_to(starts[None, :], (SUB, width))
    groups = 2 * bins // RADIX // SUB
    whole = pl.BlockSpec(memory_space=pltpu.VMEM)
    out = pl.pallas_call(
        functools.partial(kernel, bins),
        grid=(steps,),
        out_shape=jax.ShapeDtypeStruct((steps, 1, width), jnp.float32),
        in_specs=[whole] * 6,
        out_specs=pl.BlockSpec((1, 1, width), lambda i: (i, 0, 0)),
        scratch_shapes=[
            pltpu.VMEM(base.shape, jnp.float32),
            pltpu.VMEM((RADIX, groups * 2 * SUB, 2 * bins // RADIX), jnp.bfloat16),
            pltpu.VMEM((RADIX, parts * depth2, LANES), jnp.float32),
            pltpu.VMEM((groups, RADIX, 2 * SUB, width), jnp.bfloat16),
        ],
        compiler_params=pltpu.CompilerParams(vmem_limit_bytes=50 * 1024 * 1024),
    )(received, strain, jnp.asarray(base), jnp.asarray(turn), jnp.asarray(second), starts)
    out = out.reshape(tiles, segs, per_tile)
    return out.transpose(0, 2, 1).reshape(tiles * per_tile, segs)[:rows]


def join_parts(pieces, depth):
    if depth % SUB == 0:
        return pieces
    parts, _, _, last = pieces.shape
    pieces = pieces.reshape(parts, RADIX, 2, depth, last).transpose(1, 2, 0, 3, 4)
    return pieces.reshape(1, RADIX, 2 * parts * depth, last)


def share(piece, axes):
    count = lax.axis_size(axes)
    return lax.all_to_all(jnp.broadcast_to(piece[None], (count,) + piece.shape), axes, 0, 0, tiled=True)


def on_device(spectra, templates, valid_start):
    parts = lax.axis_size("freq")
    bins_here, _, rows_here = templates.shape
    depth = bins_here // RADIX
    rows = rows_here // parts
    bank = templates.reshape(depth, RADIX, 2, parts, rows).transpose(3, 1, 2, 0, 4)
    strain = share(spectra.reshape(bins_here * 2, -1).T, "group")
    segs = strain.shape[0] * strain.shape[1]
    strain = strain.reshape(segs, depth, RADIX, 2).transpose(2, 3, 1, 0)
    strain = jnp.broadcast_to(strain[None], (parts,) + strain.shape)
    bank = jnp.concatenate([bank, strain], 4)
    bank = jnp.pad(bank, ((0, 0),) * 4 + ((0, LANES - rows - segs),))
    bank = bank.reshape(parts, RADIX, 2 * depth, LANES)
    received = lax.all_to_all(bank, "freq", 0, 0, tiled=True)
    strain = received[..., rows : rows + segs]
    peaks = correlate(join_parts(received, depth), join_parts(strain, depth), valid_start, rows)
    peaks = share(peaks.reshape(1, -1), "freq")
    return peaks.reshape(rows_here, -1)


MESH = pl.DeviceIdType.MESH


def fused_tables(bins):
    base, turn, _ = tables(bins)
    groups, _, _, cols = base.shape
    base = base.reshape(groups, 2, SUB, 2, cols // (2 * SUB), SUB)
    base = base.transpose(0, 1, 2, 4, 3, 5).reshape(groups, 2, SUB, cols)
    b = np.arange(RADIX)
    angle = 2.0 * math.pi * ((b[: RADIX * 3 // 4, None] * b[None, :]) % RADIX) / RADIX
    second = rotation(angle, 0, 2) * SCALE
    second = np.kron(second.reshape(-1, 2 * RADIX), np.eye(SUB))
    return base, turn, second.astype(jnp.bfloat16)


def block_transpose(rows, size):
    count = len(rows)
    lane = lax.broadcasted_iota(jnp.int32, rows[0].shape, rows[0].ndim - 1) // size
    step = count // 2
    while step:
        low = (lane // step) % 2 == 0
        fresh = list(rows)
        for i in range(count):
            if i & step == 0:
                first, second = rows[i], rows[i + step]
                axis = first.ndim - 1
                fresh[i] = jnp.where(low, first, pltpu.roll(second, size * step, axis))
                fresh[i + step] = jnp.where(low, pltpu.roll(first, LANES - size * step, axis), second)
        rows = fresh
        step //= 2
    return rows


def corner_turn(x, size):
    row = lax.broadcasted_iota(jnp.int32, x.shape, 0)
    block = lax.broadcasted_iota(jnp.int32, x.shape, 1) // size
    step = SUB // 2
    while step:
        low, left = (row // step) % 2, (block // step) % 2
        below = pltpu.roll(pltpu.roll(x, SUB - step, 0), size * step, 1)
        above = pltpu.roll(pltpu.roll(x, step, 0), LANES - size * step, 1)
        x = jnp.where(low == left, x, jnp.where(low == 0, below, above))
        step //= 2
    return x


def fused_kernel(
    x_hbm, s_hbm, vs_ref, base_hbm, turn_hbm, w2_hbm, out_ref,
    x_ref, own_ref, send_ref, recv_ref, work_ref, turn_ref, w2_ref, w1_ref, s_ref, strain_ref, dexp_ref,
    pick_ref, cross_ref, y_ref, peak_ref,
    load_sem, table_sem, send_sem, recv_sem, ssend_sem, srecv_sem, gsend_sem, grecv_sem, psend_sem, precv_sem,
):
    tiles, parts = recv_ref.shape[:2]
    halves, highs = recv_ref.shape[2:4]
    lows = RADIX // highs
    size = LANES // parts
    segs = vs_ref.shape[0]
    width = y_ref.shape[3]
    groups = y_ref.shape[0]
    crowd = strain_ref.shape[0]
    bins_here = x_ref.shape[1]
    rows = 2 * SUB * RADIX
    lags = 2 * parts * bins_here
    inner = lags // RADIX
    quarter = lags // 4
    blocks = parts * halves
    me = lax.axis_index("freq")
    team = lax.axis_index("group")

    def others(count, here):
        return [lax.rem(here + hop, count) for hop in range(1, count)]

    def load(tile):
        return pltpu.make_async_copy(
            x_hbm.at[:, :, pl.ds(tile * LANES, LANES)], x_ref.at[tile], load_sem.at[tile]
        )

    table_copies = [
        pltpu.make_async_copy(s_hbm, own_ref, table_sem.at[0]),
        pltpu.make_async_copy(base_hbm, work_ref, table_sem.at[1]),
        pltpu.make_async_copy(turn_hbm, turn_ref, table_sem.at[2]),
        pltpu.make_async_copy(w2_hbm, w2_ref, table_sem.at[3]),
    ]
    table_copies[0].start()
    for tile in range(tiles):
        load(tile).start()
    for copy in table_copies[1:]:
        copy.start()

    barrier = pltpu.get_barrier_semaphore()
    for target in others(parts, me):
        pl.semaphore_signal(barrier, inc=1, device_id={"freq": target}, device_id_type=MESH)
    for target in others(crowd, team):
        pl.semaphore_signal(barrier, inc=1, device_id={"group": target}, device_id_type=MESH)

    def strain_copy(source, target):
        return pltpu.make_async_remote_copy(
            src_ref=s_ref, dst_ref=strain_ref.at[team, source],
            send_sem=ssend_sem.at[target], recv_sem=srecv_sem.at[source],
            device_id={"freq": target}, device_id_type=MESH,
        )

    def team_copy(source, target):
        return pltpu.make_async_remote_copy(
            src_ref=strain_ref.at[team], dst_ref=strain_ref.at[source],
            send_sem=gsend_sem.at[target], recv_sem=grecv_sem.at[source],
            device_id={"group": target}, device_id_type=MESH,
        )

    def bank_copy(tile, source, target):
        return pltpu.make_async_remote_copy(
            src_ref=send_ref.at[tile, target], dst_ref=recv_ref.at[tile, source],
            send_sem=send_sem.at[tile, target], recv_sem=recv_sem.at[tile, source],
            device_id={"freq": target}, device_id_type=MESH,
        )

    def peak_copy(source, target):
        return pltpu.make_async_remote_copy(
            src_ref=peak_ref.at[me], dst_ref=peak_ref.at[source],
            send_sem=psend_sem.at[target], recv_sem=precv_sem.at[source],
            device_id={"freq": target}, device_id_type=MESH,
        )

    place = lax.broadcasted_iota(jnp.int32, (rows, rows), 0)
    origin = ((place % SUB) * RADIX + place // (2 * SUB)) * 2 + (place // SUB) % 2
    sort = (lax.broadcasted_iota(jnp.int32, (rows, rows), 1) == origin).astype(jnp.bfloat16)

    table_copies[0].wait()
    for tile in range(tiles):
        load(tile).wait()
    place = lax.broadcasted_iota(jnp.int32, (rows, rows), 1)
    origin = ((place // SUB) % 2 * SUB + place % SUB) * RADIX + place // (2 * SUB)
    order = (lax.broadcasted_iota(jnp.int32, (rows, rows), 0) == origin).astype(jnp.bfloat16)
    span = SUB * RADIX
    strain = []
    for h in range(halves):
        piece = jnp.concatenate([own_ref[c, :, h * span : (h + 1) * span] for c in range(2)], 1)
        strain.append(jnp.dot(piece, order, preferred_element_type=jnp.float32))
    strain = jnp.concatenate(strain, 1)
    lane = lax.broadcasted_iota(jnp.int32, strain.shape, 1)
    row = lax.broadcasted_iota(jnp.int32, strain.shape, 0)
    start = jnp.zeros(strain.shape, jnp.int32)
    for s in range(strain.shape[0]):
        start = jnp.where(row == s, vs_ref[team * strain.shape[0] + s], start)
    turns = (start >= quarter).astype(jnp.int32) + (start >= 2 * quarter).astype(jnp.int32)
    turns = (turns * (lane // (2 * SUB))) % 4
    imaginary = (lane // SUB) % 2 == 1
    wide = strain.shape[1]
    swapped = jnp.where(imaginary, pltpu.roll(strain, SUB, 1), -pltpu.roll(strain, wide - SUB, 1))
    strain = jnp.where(turns % 2 == 1, swapped, strain)
    s_ref[...] = jnp.where(turns >= 2, -strain, strain).astype(jnp.bfloat16)
    for tile in range(tiles):
        x = x_ref[tile].reshape(halves, rows, LANES)
        x = jnp.stack([jnp.dot(sort, x[h], preferred_element_type=jnp.float32) for h in range(halves)])
        x = x.reshape(halves * highs, lows, 2 * SUB, LANES)
        x = block_transpose([x[:, i] for i in range(lows)], size)
        for p in range(parts):
            send_ref[tile, p] = x[p].astype(jnp.bfloat16).reshape(halves, highs, 2 * SUB, LANES)

    pl.semaphore_wait(barrier, parts + crowd - 2)
    for target in others(parts, me):
        strain_copy(me, target).start()
    for tile in range(tiles):
        for target in others(parts, me):
            bank_copy(tile, me, target).start()
    strain_ref[team, me] = s_ref[...]
    for tile in range(tiles):
        recv_ref[tile, me] = send_ref[tile, me]

    bank_row = lax.broadcasted_iota(jnp.int32, (LANES, 2 * LANES), 0)
    bank_lane = lax.broadcasted_iota(jnp.int32, (LANES, 2 * LANES), 1)
    for pair in range(lows // 2):
        wanted = (2 * pair + bank_lane // LANES) * size + bank_lane % size
        pick_ref[pair] = (bank_row == wanted).astype(jnp.bfloat16)
    collect = (bank_row % size == bank_lane % size).astype(jnp.float32)
    seg = lax.broadcasted_iota(jnp.int32, (SUB, width), 1) // size
    start = jnp.zeros((SUB, width), jnp.int32)
    for s in range(segs):
        start = jnp.where(seg == s, vs_ref[s], start)
    offset = lax.broadcasted_iota(jnp.int32, (SUB, width), 0) - start % quarter

    for copy in table_copies[1:]:
        copy.wait()

    @pl.loop(0, RADIX)
    def _(b):
        w1_ref[b] = work_ref[...].reshape(w1_ref.shape[1:]).astype(jnp.bfloat16)
        top, bottom = work_ref[:, 0], work_ref[:, 1]
        cosine, sine = turn_ref[0], turn_ref[1]
        work_ref[:, 0] = top * cosine - bottom * sine
        work_ref[:, 1] = bottom * cosine + top * sine

    for source in others(parts, me):
        strain_copy(source, source).wait_recv()
    for target in others(crowd, team):
        team_copy(team, target).start()
    for source in others(crowd, team):
        team_copy(source, source).wait_recv()

    lane_seg = lax.broadcasted_iota(jnp.int32, (segs, width), 1) // size
    spread = (lax.broadcasted_iota(jnp.int32, (segs, width), 0) == lane_seg).astype(jnp.bfloat16)
    for f in range(parts):
        piece = jnp.concatenate([strain_ref[g, f] for g in range(crowd)], 0)
        piece = lax.dot_general(
            piece, spread, (((0,), (0,)), ((), ())), preferred_element_type=jnp.float32
        )
        piece = piece.reshape(halves, RADIX, 2 * SUB, width)
        for h in range(halves):
            dexp_ref[:, f * halves + h] = piece[h]

    def expand(tile, high):
        piece = recv_ref[tile, :, :, high].reshape(blocks * 2 * SUB, LANES)
        for pair in range(lows // 2):
            bank = jnp.dot(piece, pick_ref[pair], preferred_element_type=jnp.float32)
            bank = bank.reshape(blocks, 2 * SUB, 2 * LANES)
            for k in range(2):
                b = high * lows + 2 * pair + k
                h0 = bank[:, :SUB, k * LANES : (k + 1) * LANES]
                h1 = bank[:, SUB:, k * LANES : (k + 1) * LANES]
                for side in range(width // LANES):
                    here = slice(side * LANES, (side + 1) * LANES)
                    d0, d1 = dexp_ref[b, :, :SUB, here], dexp_ref[b, :, SUB:, here]
                    cross = jnp.concatenate([h0 * d0 + h1 * d1, h0 * d1 - h1 * d0], 1)
                    cross_ref[b, :, here] = cross.reshape(blocks * 2 * SUB, LANES).astype(jnp.bfloat16)

    def transform(high):
        for i in range(lows):
            b = high * lows + i
            y = jnp.dot(w1_ref[b], cross_ref[b], preferred_element_type=jnp.float32)
            y_ref[:, b] = y.astype(jnp.bfloat16).reshape(groups, 2 * SUB, width)

    def arrive(tile):
        for source in others(parts, me):
            bank_copy(tile, source, source).wait_recv()


    @pl.loop(0, tiles)
    def _(tile):
        arrive(tile)
        for high in range(highs):
            expand(tile, high)
            transform(high)

        def add_squares(f, total):
            piece = recv_ref[tile, f].astype(jnp.float32).reshape(-1, SUB, LANES)
            return total + jnp.sum(piece * piece, 0)

        norm = jnp.zeros((SUB, LANES), jnp.float32)
        for f in range(parts):
            norm = add_squares(f, norm)
        norm = jnp.dot(norm, collect, precision=lax.Precision.HIGHEST, preferred_element_type=jnp.float32)
        norm = jnp.sum(norm, 0, keepdims=True) * (SCALE * SCALE)

        def second_stage(g, best):
            z = jnp.dot(
                w2_ref[...], y_ref[g].reshape(w2_ref.shape[1], width), preferred_element_type=jnp.float32
            )
            z = z.reshape(2, -1, SUB, width)
            for t in range(RADIX // 2):
                re, im = z[0, t], z[1, t]
                if t + RADIX // 2 < z.shape[1]:
                    inside = offset >= -(g * SUB + t * inner)
                    re = jnp.where(inside, re, z[0, t + RADIX // 2])
                    im = jnp.where(inside, im, z[1, t + RADIX // 2])
                best = jnp.maximum(best, re * re + im * im)
            return best

        best = lax.fori_loop(
            0, groups, second_stage, jnp.zeros((SUB, width), jnp.float32), unroll=32
        )
        peak_ref[me, tile] = jnp.max(best, 0, keepdims=True) / norm

    for target in others(parts, me):
        peak_copy(me, target).start()
    for source in others(parts, me):
        peak_copy(source, source).wait_recv()
    for tile in range(tiles):
        peaks = jnp.concatenate([peak_ref[p, tile] for p in range(parts)], 0)
        for side in range(width // LANES):
            out_ref[side * SUB : (side + 1) * SUB, tile * LANES : (tile + 1) * LANES] = corner_turn(
                peaks[:, side * LANES : (side + 1) * LANES], size
            )
    for target in others(parts, me):
        peak_copy(me, target).wait_send()
        strain_copy(me, target).wait_send()
        for tile in range(tiles):
            bank_copy(tile, me, target).wait_send()
    for target in others(crowd, team):
        team_copy(team, target).wait_send()


def fused(spectra, templates, valid_start):
    parts, crowd = lax.axis_size("freq"), lax.axis_size("group")
    bins_here, _, rows_here = templates.shape
    segs_here = spectra.shape[2]
    segs = segs_here * crowd
    bins = bins_here * parts
    tiles = rows_here // LANES
    halves = bins_here // (SUB * RADIX)
    highs = RADIX // parts
    width = LANES // parts * segs
    base, turn, second = fused_tables(bins)
    groups = 2 * bins // RADIX // SUB
    far = pl.BlockSpec(memory_space=pltpu.HBM)
    whole = pl.BlockSpec(memory_space=pltpu.VMEM)
    dma = pltpu.SemaphoreType.DMA
    chunk = (halves, highs, 2 * SUB, LANES)
    out = pl.pallas_call(
        fused_kernel,
        out_shape=jax.ShapeDtypeStruct((segs, rows_here), jnp.float32),
        in_specs=[far, far, pl.BlockSpec(memory_space=pltpu.SMEM), far, far, far],
        out_specs=whole,
        scratch_shapes=[
            pltpu.VMEM((tiles, bins_here, 2, LANES), jnp.bfloat16),
            pltpu.VMEM((2, segs_here, bins_here), jnp.bfloat16),
            pltpu.VMEM((tiles, parts) + chunk, jnp.bfloat16),
            pltpu.VMEM((tiles, parts) + chunk, jnp.bfloat16),
            pltpu.VMEM(base.shape, jnp.float32),
            pltpu.VMEM(turn.shape, jnp.float32),
            pltpu.VMEM(second.shape, jnp.bfloat16),
            pltpu.VMEM((RADIX, groups * 2 * SUB, 2 * bins // RADIX), jnp.bfloat16),
            pltpu.VMEM((segs_here, 2 * bins_here), jnp.bfloat16),
            pltpu.VMEM((crowd, parts, segs_here, 2 * bins_here), jnp.bfloat16),
            pltpu.VMEM((RADIX, parts * halves, 2 * SUB, width), jnp.float32),
            pltpu.VMEM((parts // 2, LANES, 2 * LANES), jnp.bfloat16),
            pltpu.VMEM((RADIX, 2 * bins // RADIX, width), jnp.bfloat16),
            pltpu.VMEM((groups, RADIX, 2 * SUB, width), jnp.bfloat16),
            pltpu.VMEM((parts, tiles, 1, width), jnp.float32),
            dma((tiles,)), dma((4,)),
            dma((tiles, parts)), dma((tiles, parts)),
            dma((parts,)), dma((parts,)),
            dma((crowd,)), dma((crowd,)),
            dma((parts,)), dma((parts,)),
        ],
        compiler_params=pltpu.CompilerParams(
            vmem_limit_bytes=60 * 1024 * 1024, collective_id=0, has_side_effects=True
        ),
    )(templates, spectra.transpose(1, 2, 0), valid_start, jnp.asarray(base), jnp.asarray(turn), jnp.asarray(second))
    return out.T


def fits(spectra, templates):
    parts = lax.axis_size("freq")
    segs = spectra.shape[2] * lax.axis_size("group")
    bins_here, _, rows_here = templates.shape
    return (
        parts == SUB
        and rows_here % LANES == 0
        and bins_here % (SUB * RADIX) == 0
        and LANES // parts * segs == 2 * LANES
    )


def dispatch(spectra, templates, valid_start):
    if fits(spectra, templates):
        return fused(spectra, templates, valid_start)
    return on_device(spectra, templates, valid_start)


def solution(mesh):
    in_specs = (P("freq", None, "group"), P("freq", None, "group"), P())
    out_specs = P("group", None)
    return jax.shard_map(
        dispatch, mesh=mesh, in_specs=in_specs, out_specs=out_specs, check_vma=False
    )
```

```python
import functools
import math

import jax
import jax.numpy as jnp
import numpy as np
from jax import lax
from jax.experimental import pallas as pl
from jax.experimental.pallas import tpu as pltpu
from jax.sharding import PartitionSpec as P

LANES = 128
RADIX = 16
SUB = 8
SCALE = 1.1328125


def rotation(angle, row_axis, col_axis):
    cosine, sine = np.cos(angle), np.sin(angle)
    top = np.stack([cosine, -sine], col_axis)
    bottom = np.stack([sine, cosine], col_axis)
    return np.stack([top, bottom], row_axis)


def tables(bins):
    lags = 2 * bins
    inner = lags // RADIX
    a = np.arange(bins // RADIX)
    tau1 = np.arange(inner)
    angle = 2.0 * math.pi * ((tau1[:, None] * a[None, :]) % inner) / inner
    first = rotation(angle.reshape(inner // SUB, SUB, a.size), 1, 2)
    first = first.reshape(inner // SUB, 2, SUB, 2 * a.size)
    turn = 2.0 * math.pi * tau1.reshape(inner // SUB, SUB, 1) / lags
    turn = np.stack([np.cos(turn), np.sin(turn)], 0)
    b = np.arange(RADIX)
    angle = 2.0 * math.pi * ((b[:, None] * b[None, :]) % RADIX) / RADIX
    second = rotation(angle, 0, 2) * SCALE
    second = second.reshape(2 * RADIX, 2 * RADIX)
    second = np.kron(second, np.eye(SUB))
    return first.astype(np.float32), turn.astype(np.float32), second.astype(jnp.bfloat16)


def kernel(valid, r_ref, d_ref, base_ref, turn_ref, w2_ref, vs_ref, out_ref, work_ref, w1_ref, dexp_ref, y_ref):
    step = pl.program_id(0)
    width = out_ref.shape[2]
    parts, _, depth2, _ = r_ref.shape
    depth = depth2 // 2
    segs = d_ref.shape[3]
    per_tile = LANES // segs
    half = parts * depth
    rows2, cols2 = w2_ref.shape
    groups = y_ref.shape[0]
    inner = groups * SUB

    @pl.when(step == 0)
    def _():
        work_ref[...] = base_ref[...]

        @pl.loop(0, RADIX)
        def _(b):
            w1_ref[b] = work_ref[...].reshape(w1_ref.shape[1:]).astype(jnp.bfloat16)
            top, bottom = work_ref[:, 0], work_ref[:, 1]
            cosine, sine = turn_ref[0], turn_ref[1]
            work_ref[:, 0] = top * cosine - bottom * sine
            work_ref[:, 1] = bottom * cosine + top * sine

        seg_spread = (
            lax.broadcasted_iota(jnp.int32, (segs, LANES), 0)
            == lax.broadcasted_iota(jnp.int32, (segs, LANES), 1) // per_tile
        ).astype(jnp.bfloat16)

        @pl.loop(0, RADIX)
        def _(b):
            piece = d_ref[:, b].reshape(2 * half, segs)
            dexp_ref[b] = jnp.dot(piece, seg_spread, preferred_element_type=jnp.float32)

    lane = lax.broadcasted_iota(jnp.int32, (LANES, width), 1)
    wanted = step * (width // segs) + (lane // LANES) * per_tile + lane % per_tile
    pick = (lax.broadcasted_iota(jnp.int32, (LANES, width), 0) == wanted).astype(jnp.bfloat16)

    def split(x):
        x = x.reshape(parts, 2, depth, x.shape[1])
        return x[:, 0].reshape(half, -1), x[:, 1].reshape(half, -1)

    def first_stage(b, norm):
        bank = jnp.dot(
            r_ref[:, b].reshape(2 * half, LANES), pick, preferred_element_type=jnp.float32
        )
        h0, h1 = split(bank)
        d0, d1 = split(dexp_ref[b])
        d0 = jnp.concatenate([d0] * (width // LANES), 1)
        d1 = jnp.concatenate([d1] * (width // LANES), 1)
        square = h0 * h0 + h1 * h1
        norm = norm + jnp.sum(square.reshape(half // SUB, SUB, width), 0)
        cross = jnp.concatenate([h0 * d0 + h1 * d1, h0 * d1 - h1 * d0], 0).astype(jnp.bfloat16)
        y = jnp.dot(w1_ref[b], cross, preferred_element_type=jnp.float32)
        y_ref[:, b] = y.astype(jnp.bfloat16).reshape(groups, 2 * SUB, width)
        return norm

    norm = lax.fori_loop(
        0, RADIX, first_stage, jnp.zeros((SUB, width), jnp.float32), unroll=2
    )
    offset = lax.broadcasted_iota(jnp.int32, (SUB, width), 0) - vs_ref[...]
    row = lax.broadcasted_iota(jnp.int32, (RADIX, SUB, width), 0) * inner

    def second_stage(g, best):
        z = jnp.dot(
            w2_ref[...], y_ref[g].reshape(cols2, width), preferred_element_type=jnp.float32
        )
        re, im = z[: rows2 // 2], z[rows2 // 2 :]
        power = (re * re + im * im).reshape(RADIX, SUB, width)
        late = row + (offset + g * SUB)[None]
        inside = (late >= 0) & (late < valid)
        return jnp.maximum(best, jnp.max(jnp.where(inside, power, 0.0), 0))

    best = lax.fori_loop(
        0, groups, second_stage, jnp.zeros((SUB, width), jnp.float32), unroll=4
    )
    norm = jnp.sum(norm, 0, keepdims=True) * (SCALE * SCALE)
    out_ref[0] = jnp.max(best, 0, keepdims=True) / norm


def correlate(received, strain, starts, rows):
    parts, _, depth2, _ = received.shape
    segs = strain.shape[3]
    bins = parts * RADIX * depth2 // 2
    base, turn, second = tables(bins)
    per_tile = LANES // segs
    tiles = -(-rows // per_tile)
    width = 2 * LANES if tiles % 2 == 0 else LANES
    steps = tiles * LANES // width
    starts = jnp.tile(jnp.repeat(starts, per_tile), width // LANES)
    starts = jnp.broadcast_to(starts[None, :], (SUB, width))
    groups = 2 * bins // RADIX // SUB
    whole = pl.BlockSpec(memory_space=pltpu.VMEM)
    out = pl.pallas_call(
        functools.partial(kernel, bins),
        grid=(steps,),
        out_shape=jax.ShapeDtypeStruct((steps, 1, width), jnp.float32),
        in_specs=[whole] * 6,
        out_specs=pl.BlockSpec((1, 1, width), lambda i: (i, 0, 0)),
        scratch_shapes=[
            pltpu.VMEM(base.shape, jnp.float32),
            pltpu.VMEM((RADIX, groups * 2 * SUB, 2 * bins // RADIX), jnp.bfloat16),
            pltpu.VMEM((RADIX, parts * depth2, LANES), jnp.float32),
            pltpu.VMEM((groups, RADIX, 2 * SUB, width), jnp.bfloat16),
        ],
        compiler_params=pltpu.CompilerParams(vmem_limit_bytes=50 * 1024 * 1024),
    )(received, strain, jnp.asarray(base), jnp.asarray(turn), jnp.asarray(second), starts)
    out = out.reshape(tiles, segs, per_tile)
    return out.transpose(0, 2, 1).reshape(tiles * per_tile, segs)[:rows]


def join_parts(pieces, depth):
    if depth % SUB == 0:
        return pieces
    parts, _, _, last = pieces.shape
    pieces = pieces.reshape(parts, RADIX, 2, depth, last).transpose(1, 2, 0, 3, 4)
    return pieces.reshape(1, RADIX, 2 * parts * depth, last)


def share(piece, axes):
    count = lax.axis_size(axes)
    return lax.all_to_all(jnp.broadcast_to(piece[None], (count,) + piece.shape), axes, 0, 0, tiled=True)


def on_device(spectra, templates, valid_start):
    parts = lax.axis_size("freq")
    bins_here, _, rows_here = templates.shape
    depth = bins_here // RADIX
    rows = rows_here // parts
    bank = templates.reshape(depth, RADIX, 2, parts, rows).transpose(3, 1, 2, 0, 4)
    strain = share(spectra.reshape(bins_here * 2, -1).T, "group")
    segs = strain.shape[0] * strain.shape[1]
    strain = strain.reshape(segs, depth, RADIX, 2).transpose(2, 3, 1, 0)
    strain = jnp.broadcast_to(strain[None], (parts,) + strain.shape)
    bank = jnp.concatenate([bank, strain], 4)
    bank = jnp.pad(bank, ((0, 0),) * 4 + ((0, LANES - rows - segs),))
    bank = bank.reshape(parts, RADIX, 2 * depth, LANES)
    received = lax.all_to_all(bank, "freq", 0, 0, tiled=True)
    strain = received[..., rows : rows + segs]
    peaks = correlate(join_parts(received, depth), join_parts(strain, depth), valid_start, rows)
    peaks = share(peaks.reshape(1, -1), "freq")
    return peaks.reshape(rows_here, -1)


MESH = pl.DeviceIdType.MESH


def fused_tables(bins):
    base, turn, _ = tables(bins)
    groups, _, _, cols = base.shape
    base = base.reshape(groups, 2, SUB, 2, cols // (2 * SUB), SUB)
    base = base.transpose(0, 1, 2, 4, 3, 5).reshape(groups, 2, SUB, cols)
    b = np.arange(RADIX)
    angle = 2.0 * math.pi * ((b[: RADIX * 3 // 4, None] * b[None, :]) % RADIX) / RADIX
    second = rotation(angle, 0, 2) * SCALE
    second = np.kron(second.reshape(-1, 2 * RADIX), np.eye(SUB))
    return base, turn, second.astype(jnp.bfloat16)


def block_transpose(rows, size):
    count = len(rows)
    lane = lax.broadcasted_iota(jnp.int32, rows[0].shape, rows[0].ndim - 1) // size
    step = count // 2
    while step:
        low = (lane // step) % 2 == 0
        fresh = list(rows)
        for i in range(count):
            if i & step == 0:
                first, second = rows[i], rows[i + step]
                axis = first.ndim - 1
                fresh[i] = jnp.where(low, first, pltpu.roll(second, size * step, axis))
                fresh[i + step] = jnp.where(low, pltpu.roll(first, LANES - size * step, axis), second)
        rows = fresh
        step //= 2
    return rows


def corner_turn(x, size):
    row = lax.broadcasted_iota(jnp.int32, x.shape, 0)
    block = lax.broadcasted_iota(jnp.int32, x.shape, 1) // size
    step = SUB // 2
    while step:
        low, left = (row // step) % 2, (block // step) % 2
        below = pltpu.roll(pltpu.roll(x, SUB - step, 0), size * step, 1)
        above = pltpu.roll(pltpu.roll(x, step, 0), LANES - size * step, 1)
        x = jnp.where(low == left, x, jnp.where(low == 0, below, above))
        step //= 2
    return x


def fused_kernel(
    x_hbm, s_hbm, vs_ref, base_hbm, turn_hbm, w2_hbm, out_ref,
    x_ref, own_ref, send_ref, recv_ref, work_ref, turn_ref, w2_ref, w1_ref, s_ref, strain_ref, dexp_ref,
    pick_ref, cross_ref, y_ref, peak_ref,
    load_sem, table_sem, send_sem, recv_sem, ssend_sem, srecv_sem, gsend_sem, grecv_sem, psend_sem, precv_sem,
):
    tiles, parts = recv_ref.shape[:2]
    halves, highs = recv_ref.shape[2:4]
    lows = RADIX // highs
    size = LANES // parts
    segs = vs_ref.shape[0]
    width = y_ref.shape[3]
    groups = y_ref.shape[0]
    crowd = strain_ref.shape[0]
    bins_here = x_ref.shape[1]
    rows = 2 * SUB * RADIX
    lags = 2 * parts * bins_here
    inner = lags // RADIX
    quarter = lags // 4
    blocks = parts * halves
    me = lax.axis_index("freq")
    team = lax.axis_index("group")

    def others(count, here):
        hops = sorted(range(1, count), key=lambda hop: (-min(hop, count - hop), hop))
        return [lax.rem(here + hop, count) for hop in hops]

    def load(tile):
        return pltpu.make_async_copy(
            x_hbm.at[:, :, pl.ds(tile * LANES, LANES)], x_ref.at[tile], load_sem.at[tile]
        )

    table_copies = [
        pltpu.make_async_copy(s_hbm, own_ref, table_sem.at[0]),
        pltpu.make_async_copy(base_hbm, work_ref, table_sem.at[1]),
        pltpu.make_async_copy(turn_hbm, turn_ref, table_sem.at[2]),
        pltpu.make_async_copy(w2_hbm, w2_ref, table_sem.at[3]),
    ]
    table_copies[0].start()
    for tile in range(tiles):
        load(tile).start()
    for copy in table_copies[1:]:
        copy.start()

    barrier = pltpu.get_barrier_semaphore()
    for target in others(parts, me):
        pl.semaphore_signal(barrier, inc=1, device_id={"freq": target}, device_id_type=MESH)
    for target in others(crowd, team):
        pl.semaphore_signal(barrier, inc=1, device_id={"group": target}, device_id_type=MESH)

    def strain_copy(source, target):
        return pltpu.make_async_remote_copy(
            src_ref=s_ref, dst_ref=strain_ref.at[team, source],
            send_sem=ssend_sem.at[target], recv_sem=srecv_sem.at[source],
            device_id={"freq": target}, device_id_type=MESH,
        )

    def team_copy(source, target):
        return pltpu.make_async_remote_copy(
            src_ref=strain_ref.at[team], dst_ref=strain_ref.at[source],
            send_sem=gsend_sem.at[target], recv_sem=grecv_sem.at[source],
            device_id={"group": target}, device_id_type=MESH,
        )

    def bank_copy(tile, source, target):
        return pltpu.make_async_remote_copy(
            src_ref=send_ref.at[tile, target], dst_ref=recv_ref.at[tile, source],
            send_sem=send_sem.at[tile, target], recv_sem=recv_sem.at[tile, source],
            device_id={"freq": target}, device_id_type=MESH,
        )

    def peak_copy(source, target):
        return pltpu.make_async_remote_copy(
            src_ref=peak_ref.at[me], dst_ref=peak_ref.at[source],
            send_sem=psend_sem.at[target], recv_sem=precv_sem.at[source],
            device_id={"freq": target}, device_id_type=MESH,
        )

    place = lax.broadcasted_iota(jnp.int32, (rows, rows), 0)
    origin = ((place % SUB) * RADIX + place // (2 * SUB)) * 2 + (place // SUB) % 2
    sort = (lax.broadcasted_iota(jnp.int32, (rows, rows), 1) == origin).astype(jnp.bfloat16)

    table_copies[0].wait()
    for tile in range(tiles):
        load(tile).wait()
    place = lax.broadcasted_iota(jnp.int32, (rows, rows), 1)
    origin = ((place // SUB) % 2 * SUB + place % SUB) * RADIX + place // (2 * SUB)
    order = (lax.broadcasted_iota(jnp.int32, (rows, rows), 0) == origin).astype(jnp.bfloat16)
    span = SUB * RADIX
    strain = []
    for h in range(halves):
        piece = jnp.concatenate([own_ref[c, :, h * span : (h + 1) * span] for c in range(2)], 1)
        strain.append(jnp.dot(piece, order, preferred_element_type=jnp.float32))
    strain = jnp.concatenate(strain, 1)
    lane = lax.broadcasted_iota(jnp.int32, strain.shape, 1)
    row = lax.broadcasted_iota(jnp.int32, strain.shape, 0)
    start = jnp.zeros(strain.shape, jnp.int32)
    for s in range(strain.shape[0]):
        start = jnp.where(row == s, vs_ref[team * strain.shape[0] + s], start)
    turns = (start >= quarter).astype(jnp.int32) + (start >= 2 * quarter).astype(jnp.int32)
    turns = (turns * (lane // (2 * SUB))) % 4
    imaginary = (lane // SUB) % 2 == 1
    wide = strain.shape[1]
    swapped = jnp.where(imaginary, pltpu.roll(strain, SUB, 1), -pltpu.roll(strain, wide - SUB, 1))
    strain = jnp.where(turns % 2 == 1, swapped, strain)
    s_ref[...] = jnp.where(turns >= 2, -strain, strain).astype(jnp.bfloat16)
    for tile in range(tiles):
        x = x_ref[tile].reshape(halves, rows, LANES)
        x = jnp.stack([jnp.dot(sort, x[h], preferred_element_type=jnp.float32) for h in range(halves)])
        x = x.reshape(halves * highs, lows, 2 * SUB, LANES)
        x = block_transpose([x[:, i] for i in range(lows)], size)
        for p in range(parts):
            send_ref[tile, p] = x[p].astype(jnp.bfloat16).reshape(halves, highs, 2 * SUB, LANES)

    pl.semaphore_wait(barrier, parts + crowd - 2)
    for target in others(parts, me):
        strain_copy(me, target).start()
    for tile in range(tiles):
        for target in others(parts, me):
            bank_copy(tile, me, target).start()
    strain_ref[team, me] = s_ref[...]
    for tile in range(tiles):
        recv_ref[tile, me] = send_ref[tile, me]

    bank_row = lax.broadcasted_iota(jnp.int32, (LANES, 2 * LANES), 0)
    bank_lane = lax.broadcasted_iota(jnp.int32, (LANES, 2 * LANES), 1)
    for pair in range(lows // 2):
        wanted = (2 * pair + bank_lane // LANES) * size + bank_lane % size
        pick_ref[pair] = (bank_row == wanted).astype(jnp.bfloat16)
    collect = (bank_row % size == bank_lane % size).astype(jnp.float32)
    seg = lax.broadcasted_iota(jnp.int32, (SUB, width), 1) // size
    start = jnp.zeros((SUB, width), jnp.int32)
    for s in range(segs):
        start = jnp.where(seg == s, vs_ref[s], start)
    offset = lax.broadcasted_iota(jnp.int32, (SUB, width), 0) - start % quarter

    for copy in table_copies[1:]:
        copy.wait()

    @pl.loop(0, RADIX)
    def _(b):
        w1_ref[b] = work_ref[...].reshape(w1_ref.shape[1:]).astype(jnp.bfloat16)
        top, bottom = work_ref[:, 0], work_ref[:, 1]
        cosine, sine = turn_ref[0], turn_ref[1]
        work_ref[:, 0] = top * cosine - bottom * sine
        work_ref[:, 1] = bottom * cosine + top * sine

    for source in others(parts, me):
        strain_copy(source, source).wait_recv()
    for target in others(crowd, team):
        team_copy(team, target).start()
    for source in others(crowd, team):
        team_copy(source, source).wait_recv()

    lane_seg = lax.broadcasted_iota(jnp.int32, (segs, width), 1) // size
    spread = (lax.broadcasted_iota(jnp.int32, (segs, width), 0) == lane_seg).astype(jnp.bfloat16)
    for f in range(parts):
        piece = jnp.concatenate([strain_ref[g, f] for g in range(crowd)], 0)
        piece = lax.dot_general(
            piece, spread, (((0,), (0,)), ((), ())), preferred_element_type=jnp.float32
        )
        piece = piece.reshape(halves, RADIX, 2 * SUB, width)
        for h in range(halves):
            dexp_ref[:, f * halves + h] = piece[h]

    def expand(tile, high, pair):
        piece = recv_ref[tile, :, :, high].reshape(blocks * 2 * SUB, LANES)
        bank = jnp.dot(piece, pick_ref[pair], preferred_element_type=jnp.float32)
        bank = bank.reshape(blocks, 2 * SUB, 2 * LANES)
        for k in range(2):
            b = high * lows + 2 * pair + k
            h0 = bank[:, :SUB, k * LANES : (k + 1) * LANES]
            h1 = bank[:, SUB:, k * LANES : (k + 1) * LANES]
            for side in range(width // LANES):
                here = slice(side * LANES, (side + 1) * LANES)
                d0, d1 = dexp_ref[b, :, :SUB, here], dexp_ref[b, :, SUB:, here]
                cross = jnp.concatenate([h0 * d0 + h1 * d1, h0 * d1 - h1 * d0], 1)
                cross_ref[b, :, here] = cross.reshape(blocks * 2 * SUB, LANES).astype(jnp.bfloat16)

    def transform(high, pair):
        for k in range(2):
            b = high * lows + 2 * pair + k
            y = jnp.dot(w1_ref[b], cross_ref[b], preferred_element_type=jnp.float32)
            y_ref[:, b] = y.astype(jnp.bfloat16).reshape(groups, 2 * SUB, width)

    def arrive(tile):
        for source in others(parts, me):
            bank_copy(tile, source, source).wait_recv()


    @pl.loop(0, tiles)
    def _(tile):
        arrive(tile)
        pairs = [(high, pair) for high in range(highs) for pair in range(lows // 2)]
        expand(tile, *pairs[0])
        for now, later in zip(pairs, pairs[1:] + [None]):
            if later is not None:
                expand(tile, *later)
            transform(*now)

        def add_squares(f, total):
            piece = recv_ref[tile, f].astype(jnp.float32).reshape(-1, SUB, LANES)
            return total + jnp.sum(piece * piece, 0)

        norm = jnp.zeros((SUB, LANES), jnp.float32)
        for f in range(parts):
            norm = add_squares(f, norm)
        norm = jnp.dot(norm, collect, precision=lax.Precision.HIGHEST, preferred_element_type=jnp.float32)
        norm = jnp.sum(norm, 0, keepdims=True) * (SCALE * SCALE)

        def second_stage(g, best):
            z = jnp.dot(
                w2_ref[...], y_ref[g].reshape(w2_ref.shape[1], width), preferred_element_type=jnp.float32
            )
            z = z.reshape(2, -1, SUB, width)
            for t in range(RADIX // 2):
                re, im = z[0, t], z[1, t]
                if t + RADIX // 2 < z.shape[1]:
                    inside = offset >= -(g * SUB + t * inner)
                    re = jnp.where(inside, re, z[0, t + RADIX // 2])
                    im = jnp.where(inside, im, z[1, t + RADIX // 2])
                best = jnp.maximum(best, re * re + im * im)
            return best

        best = lax.fori_loop(
            0, groups, second_stage, jnp.zeros((SUB, width), jnp.float32), unroll=32
        )
        peak_ref[me, tile] = jnp.max(best, 0, keepdims=True) / norm

    for target in others(parts, me):
        peak_copy(me, target).start()
    for target in others(parts, me):
        strain_copy(me, target).wait_send()
        for tile in range(tiles):
            bank_copy(tile, me, target).wait_send()
    for target in others(crowd, team):
        team_copy(team, target).wait_send()
    for source in others(parts, me):
        peak_copy(source, source).wait_recv()
    for tile in range(tiles):
        peaks = jnp.concatenate([peak_ref[p, tile] for p in range(parts)], 0)
        for side in range(width // LANES):
            out_ref[side * SUB : (side + 1) * SUB, tile * LANES : (tile + 1) * LANES] = corner_turn(
                peaks[:, side * LANES : (side + 1) * LANES], size
            )
    for target in others(parts, me):
        peak_copy(me, target).wait_send()


def fused(spectra, templates, valid_start):
    parts, crowd = lax.axis_size("freq"), lax.axis_size("group")
    bins_here, _, rows_here = templates.shape
    segs_here = spectra.shape[2]
    segs = segs_here * crowd
    bins = bins_here * parts
    tiles = rows_here // LANES
    halves = bins_here // (SUB * RADIX)
    highs = RADIX // parts
    width = LANES // parts * segs
    base, turn, second = fused_tables(bins)
    groups = 2 * bins // RADIX // SUB
    far = pl.BlockSpec(memory_space=pltpu.HBM)
    whole = pl.BlockSpec(memory_space=pltpu.VMEM)
    dma = pltpu.SemaphoreType.DMA
    chunk = (halves, highs, 2 * SUB, LANES)
    out = pl.pallas_call(
        fused_kernel,
        out_shape=jax.ShapeDtypeStruct((segs, rows_here), jnp.float32),
        in_specs=[far, far, pl.BlockSpec(memory_space=pltpu.SMEM), far, far, far],
        out_specs=whole,
        scratch_shapes=[
            pltpu.VMEM((tiles, bins_here, 2, LANES), jnp.bfloat16),
            pltpu.VMEM((2, segs_here, bins_here), jnp.bfloat16),
            pltpu.VMEM((tiles, parts) + chunk, jnp.bfloat16),
            pltpu.VMEM((tiles, parts) + chunk, jnp.bfloat16),
            pltpu.VMEM(base.shape, jnp.float32),
            pltpu.VMEM(turn.shape, jnp.float32),
            pltpu.VMEM(second.shape, jnp.bfloat16),
            pltpu.VMEM((RADIX, groups * 2 * SUB, 2 * bins // RADIX), jnp.bfloat16),
            pltpu.VMEM((segs_here, 2 * bins_here), jnp.bfloat16),
            pltpu.VMEM((crowd, parts, segs_here, 2 * bins_here), jnp.bfloat16),
            pltpu.VMEM((RADIX, parts * halves, 2 * SUB, width), jnp.float32),
            pltpu.VMEM((parts // 2, LANES, 2 * LANES), jnp.bfloat16),
            pltpu.VMEM((RADIX, 2 * bins // RADIX, width), jnp.bfloat16),
            pltpu.VMEM((groups, RADIX, 2 * SUB, width), jnp.bfloat16),
            pltpu.VMEM((parts, tiles, 1, width), jnp.float32),
            dma((tiles,)), dma((4,)),
            dma((tiles, parts)), dma((tiles, parts)),
            dma((parts,)), dma((parts,)),
            dma((crowd,)), dma((crowd,)),
            dma((parts,)), dma((parts,)),
        ],
        compiler_params=pltpu.CompilerParams(
            vmem_limit_bytes=56 * 1024 * 1024, collective_id=0, has_side_effects=True
        ),
    )(templates, spectra.transpose(1, 2, 0), valid_start, jnp.asarray(base), jnp.asarray(turn), jnp.asarray(second))
    return out.T


def fits(spectra, templates):
    parts = lax.axis_size("freq")
    segs = spectra.shape[2] * lax.axis_size("group")
    bins_here, _, rows_here = templates.shape
    return (
        parts == SUB
        and rows_here % LANES == 0
        and bins_here % (SUB * RADIX) == 0
        and LANES // parts * segs == 2 * LANES
    )


def dispatch(spectra, templates, valid_start):
    if fits(spectra, templates):
        return fused(spectra, templates, valid_start)
    return on_device(spectra, templates, valid_start)


def solution(mesh):
    in_specs = (P("freq", None, "group"), P("freq", None, "group"), P())
    out_specs = P("group", None)
    return jax.shard_map(
        dispatch, mesh=mesh, in_specs=in_specs, out_specs=out_specs, check_vma=False
    )
```

```python
import functools
import math

import jax
import jax.numpy as jnp
import numpy as np
from jax import lax
from jax.experimental import pallas as pl
from jax.experimental.pallas import tpu as pltpu
from jax.sharding import PartitionSpec as P

LANES = 128
RADIX = 16
SUB = 8
SCALE = 1.1328125
AHEAD = 3


def rotation(angle, row_axis, col_axis):
    cosine, sine = np.cos(angle), np.sin(angle)
    top = np.stack([cosine, -sine], col_axis)
    bottom = np.stack([sine, cosine], col_axis)
    return np.stack([top, bottom], row_axis)


def tables(bins):
    lags = 2 * bins
    inner = lags // RADIX
    a = np.arange(bins // RADIX)
    tau1 = np.arange(inner)
    angle = 2.0 * math.pi * ((tau1[:, None] * a[None, :]) % inner) / inner
    first = rotation(angle.reshape(inner // SUB, SUB, a.size), 1, 2)
    first = first.reshape(inner // SUB, 2, SUB, 2 * a.size)
    turn = 2.0 * math.pi * tau1.reshape(inner // SUB, SUB, 1) / lags
    turn = np.stack([np.cos(turn), np.sin(turn)], 0)
    b = np.arange(RADIX)
    angle = 2.0 * math.pi * ((b[:, None] * b[None, :]) % RADIX) / RADIX
    second = rotation(angle, 0, 2) * SCALE
    second = second.reshape(2 * RADIX, 2 * RADIX)
    second = np.kron(second, np.eye(SUB))
    return first.astype(np.float32), turn.astype(np.float32), second.astype(jnp.bfloat16)


def kernel(valid, r_ref, d_ref, base_ref, turn_ref, w2_ref, vs_ref, out_ref, work_ref, w1_ref, dexp_ref, y_ref):
    step = pl.program_id(0)
    width = out_ref.shape[2]
    parts, _, depth2, _ = r_ref.shape
    depth = depth2 // 2
    segs = d_ref.shape[3]
    per_tile = LANES // segs
    half = parts * depth
    rows2, cols2 = w2_ref.shape
    groups = y_ref.shape[0]
    inner = groups * SUB

    @pl.when(step == 0)
    def _():
        work_ref[...] = base_ref[...]

        @pl.loop(0, RADIX)
        def _(b):
            w1_ref[b] = work_ref[...].reshape(w1_ref.shape[1:]).astype(jnp.bfloat16)
            top, bottom = work_ref[:, 0], work_ref[:, 1]
            cosine, sine = turn_ref[0], turn_ref[1]
            work_ref[:, 0] = top * cosine - bottom * sine
            work_ref[:, 1] = bottom * cosine + top * sine

        seg_spread = (
            lax.broadcasted_iota(jnp.int32, (segs, LANES), 0)
            == lax.broadcasted_iota(jnp.int32, (segs, LANES), 1) // per_tile
        ).astype(jnp.bfloat16)

        @pl.loop(0, RADIX)
        def _(b):
            piece = d_ref[:, b].reshape(2 * half, segs)
            dexp_ref[b] = jnp.dot(piece, seg_spread, preferred_element_type=jnp.float32)

    lane = lax.broadcasted_iota(jnp.int32, (LANES, width), 1)
    wanted = step * (width // segs) + (lane // LANES) * per_tile + lane % per_tile
    pick = (lax.broadcasted_iota(jnp.int32, (LANES, width), 0) == wanted).astype(jnp.bfloat16)

    def split(x):
        x = x.reshape(parts, 2, depth, x.shape[1])
        return x[:, 0].reshape(half, -1), x[:, 1].reshape(half, -1)

    def first_stage(b, norm):
        bank = jnp.dot(
            r_ref[:, b].reshape(2 * half, LANES), pick, preferred_element_type=jnp.float32
        )
        h0, h1 = split(bank)
        d0, d1 = split(dexp_ref[b])
        d0 = jnp.concatenate([d0] * (width // LANES), 1)
        d1 = jnp.concatenate([d1] * (width // LANES), 1)
        square = h0 * h0 + h1 * h1
        norm = norm + jnp.sum(square.reshape(half // SUB, SUB, width), 0)
        cross = jnp.concatenate([h0 * d0 + h1 * d1, h0 * d1 - h1 * d0], 0).astype(jnp.bfloat16)
        y = jnp.dot(w1_ref[b], cross, preferred_element_type=jnp.float32)
        y_ref[:, b] = y.astype(jnp.bfloat16).reshape(groups, 2 * SUB, width)
        return norm

    norm = lax.fori_loop(
        0, RADIX, first_stage, jnp.zeros((SUB, width), jnp.float32), unroll=2
    )
    offset = lax.broadcasted_iota(jnp.int32, (SUB, width), 0) - vs_ref[...]
    row = lax.broadcasted_iota(jnp.int32, (RADIX, SUB, width), 0) * inner

    def second_stage(g, best):
        z = jnp.dot(
            w2_ref[...], y_ref[g].reshape(cols2, width), preferred_element_type=jnp.float32
        )
        re, im = z[: rows2 // 2], z[rows2 // 2 :]
        power = (re * re + im * im).reshape(RADIX, SUB, width)
        late = row + (offset + g * SUB)[None]
        inside = (late >= 0) & (late < valid)
        return jnp.maximum(best, jnp.max(jnp.where(inside, power, 0.0), 0))

    best = lax.fori_loop(
        0, groups, second_stage, jnp.zeros((SUB, width), jnp.float32), unroll=4
    )
    norm = jnp.sum(norm, 0, keepdims=True) * (SCALE * SCALE)
    out_ref[0] = jnp.max(best, 0, keepdims=True) / norm


def correlate(received, strain, starts, rows):
    parts, _, depth2, _ = received.shape
    segs = strain.shape[3]
    bins = parts * RADIX * depth2 // 2
    base, turn, second = tables(bins)
    per_tile = LANES // segs
    tiles = -(-rows // per_tile)
    width = 2 * LANES if tiles % 2 == 0 else LANES
    steps = tiles * LANES // width
    starts = jnp.tile(jnp.repeat(starts, per_tile), width // LANES)
    starts = jnp.broadcast_to(starts[None, :], (SUB, width))
    groups = 2 * bins // RADIX // SUB
    whole = pl.BlockSpec(memory_space=pltpu.VMEM)
    out = pl.pallas_call(
        functools.partial(kernel, bins),
        grid=(steps,),
        out_shape=jax.ShapeDtypeStruct((steps, 1, width), jnp.float32),
        in_specs=[whole] * 6,
        out_specs=pl.BlockSpec((1, 1, width), lambda i: (i, 0, 0)),
        scratch_shapes=[
            pltpu.VMEM(base.shape, jnp.float32),
            pltpu.VMEM((RADIX, groups * 2 * SUB, 2 * bins // RADIX), jnp.bfloat16),
            pltpu.VMEM((RADIX, parts * depth2, LANES), jnp.float32),
            pltpu.VMEM((groups, RADIX, 2 * SUB, width), jnp.bfloat16),
        ],
        compiler_params=pltpu.CompilerParams(vmem_limit_bytes=50 * 1024 * 1024),
    )(received, strain, jnp.asarray(base), jnp.asarray(turn), jnp.asarray(second), starts)
    out = out.reshape(tiles, segs, per_tile)
    return out.transpose(0, 2, 1).reshape(tiles * per_tile, segs)[:rows]


def join_parts(pieces, depth):
    if depth % SUB == 0:
        return pieces
    parts, _, _, last = pieces.shape
    pieces = pieces.reshape(parts, RADIX, 2, depth, last).transpose(1, 2, 0, 3, 4)
    return pieces.reshape(1, RADIX, 2 * parts * depth, last)


def share(piece, axes):
    count = lax.axis_size(axes)
    return lax.all_to_all(jnp.broadcast_to(piece[None], (count,) + piece.shape), axes, 0, 0, tiled=True)


def on_device(spectra, templates, valid_start):
    parts = lax.axis_size("freq")
    bins_here, _, rows_here = templates.shape
    depth = bins_here // RADIX
    rows = rows_here // parts
    bank = templates.reshape(depth, RADIX, 2, parts, rows).transpose(3, 1, 2, 0, 4)
    strain = share(spectra.reshape(bins_here * 2, -1).T, "group")
    segs = strain.shape[0] * strain.shape[1]
    strain = strain.reshape(segs, depth, RADIX, 2).transpose(2, 3, 1, 0)
    strain = jnp.broadcast_to(strain[None], (parts,) + strain.shape)
    bank = jnp.concatenate([bank, strain], 4)
    bank = jnp.pad(bank, ((0, 0),) * 4 + ((0, LANES - rows - segs),))
    bank = bank.reshape(parts, RADIX, 2 * depth, LANES)
    received = lax.all_to_all(bank, "freq", 0, 0, tiled=True)
    strain = received[..., rows : rows + segs]
    peaks = correlate(join_parts(received, depth), join_parts(strain, depth), valid_start, rows)
    peaks = share(peaks.reshape(1, -1), "freq")
    return peaks.reshape(rows_here, -1)


MESH = pl.DeviceIdType.MESH


def fused_tables(bins):
    base, turn, _ = tables(bins)
    groups, _, _, cols = base.shape
    base = base.reshape(groups, 2, SUB, 2, cols // (2 * SUB), SUB)
    base = base.transpose(0, 1, 2, 4, 3, 5).reshape(groups, 2, SUB, cols)
    b = np.arange(RADIX)
    angle = 2.0 * math.pi * ((b[: RADIX * 3 // 4, None] * b[None, :]) % RADIX) / RADIX
    second = rotation(angle, 0, 2) * SCALE
    second = np.kron(second.reshape(-1, 2 * RADIX), np.eye(SUB))
    return base, turn, second.astype(jnp.bfloat16)


def block_transpose(rows, size):
    count = len(rows)
    lane = lax.broadcasted_iota(jnp.int32, rows[0].shape, rows[0].ndim - 1) // size
    step = count // 2
    while step:
        low = (lane // step) % 2 == 0
        fresh = list(rows)
        for i in range(count):
            if i & step == 0:
                first, second = rows[i], rows[i + step]
                axis = first.ndim - 1
                fresh[i] = jnp.where(low, first, pltpu.roll(second, size * step, axis))
                fresh[i + step] = jnp.where(low, pltpu.roll(first, LANES - size * step, axis), second)
        rows = fresh
        step //= 2
    return rows


def corner_turn(x, size):
    row = lax.broadcasted_iota(jnp.int32, x.shape, 0)
    block = lax.broadcasted_iota(jnp.int32, x.shape, 1) // size
    step = SUB // 2
    while step:
        low, left = (row // step) % 2, (block // step) % 2
        below = pltpu.roll(pltpu.roll(x, SUB - step, 0), size * step, 1)
        above = pltpu.roll(pltpu.roll(x, step, 0), LANES - size * step, 1)
        x = jnp.where(low == left, x, jnp.where(low == 0, below, above))
        step //= 2
    return x


def fused_kernel(
    x_hbm, s_hbm, vs_ref, base_hbm, turn_hbm, w2_hbm, out_ref,
    x_ref, own_ref, send_ref, recv_ref, work_ref, turn_ref, w2_ref, w1_ref, s_ref, strain_ref, dexp_ref,
    pick_ref, cross_ref, y_ref, peak_ref,
    load_sem, table_sem, send_sem, recv_sem, ssend_sem, srecv_sem, gsend_sem, grecv_sem, psend_sem, precv_sem,
):
    tiles, parts = recv_ref.shape[:2]
    halves, highs = recv_ref.shape[2:4]
    lows = RADIX // highs
    size = LANES // parts
    segs = vs_ref.shape[0]
    width = y_ref.shape[3]
    groups = y_ref.shape[0]
    crowd = strain_ref.shape[0]
    bins_here = x_ref.shape[1]
    rows = 2 * SUB * RADIX
    lags = 2 * parts * bins_here
    inner = lags // RADIX
    quarter = lags // 4
    blocks = parts * halves
    me = lax.axis_index("freq")
    team = lax.axis_index("group")

    def others(count, here):
        hops = sorted(range(1, count), key=lambda hop: (-min(hop, count - hop), hop))
        return [lax.rem(here + hop, count) for hop in hops]

    def load(tile):
        return pltpu.make_async_copy(
            x_hbm.at[:, :, pl.ds(tile * LANES, LANES)], x_ref.at[tile], load_sem.at[tile]
        )

    table_copies = [
        pltpu.make_async_copy(s_hbm, own_ref, table_sem.at[0]),
        pltpu.make_async_copy(base_hbm, work_ref, table_sem.at[1]),
        pltpu.make_async_copy(turn_hbm, turn_ref, table_sem.at[2]),
        pltpu.make_async_copy(w2_hbm, w2_ref, table_sem.at[3]),
    ]
    table_copies[0].start()
    for tile in range(tiles):
        load(tile).start()
    for copy in table_copies[1:]:
        copy.start()

    barrier = pltpu.get_barrier_semaphore()
    for target in others(parts, me):
        pl.semaphore_signal(barrier, inc=1, device_id={"freq": target}, device_id_type=MESH)
    for target in others(crowd, team):
        pl.semaphore_signal(barrier, inc=1, device_id={"group": target}, device_id_type=MESH)

    def strain_copy(source, target):
        return pltpu.make_async_remote_copy(
            src_ref=s_ref, dst_ref=strain_ref.at[team, source],
            send_sem=ssend_sem.at[target], recv_sem=srecv_sem.at[source],
            device_id={"freq": target}, device_id_type=MESH,
        )

    def team_copy(source, target):
        return pltpu.make_async_remote_copy(
            src_ref=strain_ref.at[team], dst_ref=strain_ref.at[source],
            send_sem=gsend_sem.at[target], recv_sem=grecv_sem.at[source],
            device_id={"group": target}, device_id_type=MESH,
        )

    def bank_copy(tile, source, target):
        return pltpu.make_async_remote_copy(
            src_ref=send_ref.at[tile, target], dst_ref=recv_ref.at[tile, source],
            send_sem=send_sem.at[tile, target], recv_sem=recv_sem.at[tile, source],
            device_id={"freq": target}, device_id_type=MESH,
        )

    def peak_copy(source, target):
        return pltpu.make_async_remote_copy(
            src_ref=peak_ref.at[me], dst_ref=peak_ref.at[source],
            send_sem=psend_sem.at[target], recv_sem=precv_sem.at[source],
            device_id={"freq": target}, device_id_type=MESH,
        )

    place = lax.broadcasted_iota(jnp.int32, (rows, rows), 0)
    origin = ((place % SUB) * RADIX + place // (2 * SUB)) * 2 + (place // SUB) % 2
    sort = (lax.broadcasted_iota(jnp.int32, (rows, rows), 1) == origin).astype(jnp.bfloat16)

    table_copies[0].wait()
    for tile in range(tiles):
        load(tile).wait()
    place = lax.broadcasted_iota(jnp.int32, (rows, rows), 1)
    origin = ((place // SUB) % 2 * SUB + place % SUB) * RADIX + place // (2 * SUB)
    order = (lax.broadcasted_iota(jnp.int32, (rows, rows), 0) == origin).astype(jnp.bfloat16)
    span = SUB * RADIX
    strain = []
    for h in range(halves):
        piece = jnp.concatenate([own_ref[c, :, h * span : (h + 1) * span] for c in range(2)], 1)
        strain.append(jnp.dot(piece, order, preferred_element_type=jnp.float32))
    strain = jnp.concatenate(strain, 1)
    lane = lax.broadcasted_iota(jnp.int32, strain.shape, 1)
    row = lax.broadcasted_iota(jnp.int32, strain.shape, 0)
    start = jnp.zeros(strain.shape, jnp.int32)
    for s in range(strain.shape[0]):
        start = jnp.where(row == s, vs_ref[team * strain.shape[0] + s], start)
    turns = (start >= quarter).astype(jnp.int32) + (start >= 2 * quarter).astype(jnp.int32)
    turns = (turns * (lane // (2 * SUB))) % 4
    imaginary = (lane // SUB) % 2 == 1
    wide = strain.shape[1]
    swapped = jnp.where(imaginary, pltpu.roll(strain, SUB, 1), -pltpu.roll(strain, wide - SUB, 1))
    strain = jnp.where(turns % 2 == 1, swapped, strain)
    s_ref[...] = jnp.where(turns >= 2, -strain, strain).astype(jnp.bfloat16)
    for tile in range(tiles):
        x = x_ref[tile].reshape(halves, rows, LANES)
        x = jnp.stack([jnp.dot(sort, x[h], preferred_element_type=jnp.float32) for h in range(halves)])
        x = x.reshape(halves * highs, lows, 2 * SUB, LANES)
        x = block_transpose([x[:, i] for i in range(lows)], size)
        for p in range(parts):
            send_ref[tile, p] = x[p].astype(jnp.bfloat16).reshape(halves, highs, 2 * SUB, LANES)

    pl.semaphore_wait(barrier, parts + crowd - 2)
    for target in others(parts, me):
        strain_copy(me, target).start()
    ahead = min(AHEAD, tiles)
    for tile in range(ahead):
        for target in others(parts, me):
            bank_copy(tile, me, target).start()
    strain_ref[team, me] = s_ref[...]
    for tile in range(tiles):
        recv_ref[tile, me] = send_ref[tile, me]

    bank_row = lax.broadcasted_iota(jnp.int32, (LANES, 2 * LANES), 0)
    bank_lane = lax.broadcasted_iota(jnp.int32, (LANES, 2 * LANES), 1)
    for pair in range(lows // 2):
        wanted = (2 * pair + bank_lane // LANES) * size + bank_lane % size
        pick_ref[pair] = (bank_row == wanted).astype(jnp.bfloat16)
    collect = (bank_row % size == bank_lane % size).astype(jnp.float32)
    seg = lax.broadcasted_iota(jnp.int32, (SUB, width), 1) // size
    start = jnp.zeros((SUB, width), jnp.int32)
    for s in range(segs):
        start = jnp.where(seg == s, vs_ref[s], start)
    offset = lax.broadcasted_iota(jnp.int32, (SUB, width), 0) - start % quarter

    for copy in table_copies[1:]:
        copy.wait()

    @pl.loop(0, RADIX)
    def _(b):
        w1_ref[b] = work_ref[...].reshape(w1_ref.shape[1:]).astype(jnp.bfloat16)
        top, bottom = work_ref[:, 0], work_ref[:, 1]
        cosine, sine = turn_ref[0], turn_ref[1]
        work_ref[:, 0] = top * cosine - bottom * sine
        work_ref[:, 1] = bottom * cosine + top * sine

    for source in others(parts, me):
        strain_copy(source, source).wait_recv()
    for target in others(crowd, team):
        team_copy(team, target).start()
    for source in others(crowd, team):
        team_copy(source, source).wait_recv()

    lane_seg = lax.broadcasted_iota(jnp.int32, (segs, width), 1) // size
    spread = (lax.broadcasted_iota(jnp.int32, (segs, width), 0) == lane_seg).astype(jnp.bfloat16)
    for f in range(parts):
        piece = jnp.concatenate([strain_ref[g, f] for g in range(crowd)], 0)
        piece = lax.dot_general(
            piece, spread, (((0,), (0,)), ((), ())), preferred_element_type=jnp.float32
        )
        piece = piece.reshape(halves, RADIX, 2 * SUB, width)
        for h in range(halves):
            dexp_ref[:, f * halves + h] = piece[h]

    def expand(tile, high, pair):
        piece = recv_ref[tile, :, :, high].reshape(blocks * 2 * SUB, LANES)
        bank = jnp.dot(piece, pick_ref[pair], preferred_element_type=jnp.float32)
        bank = bank.reshape(blocks, 2 * SUB, 2 * LANES)
        for k in range(2):
            b = high * lows + 2 * pair + k
            h0 = bank[:, :SUB, k * LANES : (k + 1) * LANES]
            h1 = bank[:, SUB:, k * LANES : (k + 1) * LANES]
            for side in range(width // LANES):
                here = slice(side * LANES, (side + 1) * LANES)
                d0, d1 = dexp_ref[b, :, :SUB, here], dexp_ref[b, :, SUB:, here]
                cross = jnp.concatenate([h0 * d0 + h1 * d1, h0 * d1 - h1 * d0], 1)
                cross_ref[b, :, here] = cross.reshape(blocks * 2 * SUB, LANES).astype(jnp.bfloat16)

    def transform(high, pair):
        for k in range(2):
            b = high * lows + 2 * pair + k
            y = jnp.dot(w1_ref[b], cross_ref[b], preferred_element_type=jnp.float32)
            y_ref[:, b] = y.astype(jnp.bfloat16).reshape(groups, 2 * SUB, width)

    def arrive(tile):
        for source in others(parts, me):
            bank_copy(tile, source, source).wait_recv()


    @pl.loop(0, tiles)
    def _(tile):
        arrive(tile)

        @pl.when(tile + ahead < tiles)
        def _():
            for target in others(parts, me):
                bank_copy(tile + ahead, me, target).start()

        pairs = [(high, pair) for high in range(highs) for pair in range(lows // 2)]
        expand(tile, *pairs[0])
        for now, later in zip(pairs, pairs[1:] + [None]):
            if later is not None:
                expand(tile, *later)
            transform(*now)

        def add_squares(f, total):
            piece = recv_ref[tile, f].astype(jnp.float32).reshape(-1, SUB, LANES)
            return total + jnp.sum(piece * piece, 0)

        norm = jnp.zeros((SUB, LANES), jnp.float32)
        for f in range(parts):
            norm = add_squares(f, norm)
        norm = jnp.dot(norm, collect, precision=lax.Precision.HIGHEST, preferred_element_type=jnp.float32)
        norm = jnp.sum(norm, 0, keepdims=True) * (SCALE * SCALE)

        def second_stage(g, best):
            z = jnp.dot(
                w2_ref[...], y_ref[g].reshape(w2_ref.shape[1], width), preferred_element_type=jnp.float32
            )
            z = z.reshape(2, -1, SUB, width)
            for t in range(RADIX // 2):
                re, im = z[0, t], z[1, t]
                if t + RADIX // 2 < z.shape[1]:
                    inside = offset >= -(g * SUB + t * inner)
                    re = jnp.where(inside, re, z[0, t + RADIX // 2])
                    im = jnp.where(inside, im, z[1, t + RADIX // 2])
                best = jnp.maximum(best, re * re + im * im)
            return best

        best = lax.fori_loop(
            0, groups, second_stage, jnp.zeros((SUB, width), jnp.float32), unroll=32
        )
        peak_ref[me, tile] = jnp.max(best, 0, keepdims=True) / norm

    for target in others(parts, me):
        peak_copy(me, target).start()
    for target in others(parts, me):
        strain_copy(me, target).wait_send()
        for tile in range(tiles):
            bank_copy(tile, me, target).wait_send()
    for target in others(crowd, team):
        team_copy(team, target).wait_send()
    for source in others(parts, me):
        peak_copy(source, source).wait_recv()
    for tile in range(tiles):
        peaks = jnp.concatenate([peak_ref[p, tile] for p in range(parts)], 0)
        for side in range(width // LANES):
            out_ref[side * SUB : (side + 1) * SUB, tile * LANES : (tile + 1) * LANES] = corner_turn(
                peaks[:, side * LANES : (side + 1) * LANES], size
            )
    for target in others(parts, me):
        peak_copy(me, target).wait_send()


def fused(spectra, templates, valid_start):
    parts, crowd = lax.axis_size("freq"), lax.axis_size("group")
    bins_here, _, rows_here = templates.shape
    segs_here = spectra.shape[2]
    segs = segs_here * crowd
    bins = bins_here * parts
    tiles = rows_here // LANES
    halves = bins_here // (SUB * RADIX)
    highs = RADIX // parts
    width = LANES // parts * segs
    base, turn, second = fused_tables(bins)
    groups = 2 * bins // RADIX // SUB
    far = pl.BlockSpec(memory_space=pltpu.HBM)
    whole = pl.BlockSpec(memory_space=pltpu.VMEM)
    dma = pltpu.SemaphoreType.DMA
    chunk = (halves, highs, 2 * SUB, LANES)
    out = pl.pallas_call(
        fused_kernel,
        out_shape=jax.ShapeDtypeStruct((segs, rows_here), jnp.float32),
        in_specs=[far, far, pl.BlockSpec(memory_space=pltpu.SMEM), far, far, far],
        out_specs=whole,
        scratch_shapes=[
            pltpu.VMEM((tiles, bins_here, 2, LANES), jnp.bfloat16),
            pltpu.VMEM((2, segs_here, bins_here), jnp.bfloat16),
            pltpu.VMEM((tiles, parts) + chunk, jnp.bfloat16),
            pltpu.VMEM((tiles, parts) + chunk, jnp.bfloat16),
            pltpu.VMEM(base.shape, jnp.float32),
            pltpu.VMEM(turn.shape, jnp.float32),
            pltpu.VMEM(second.shape, jnp.bfloat16),
            pltpu.VMEM((RADIX, groups * 2 * SUB, 2 * bins // RADIX), jnp.bfloat16),
            pltpu.VMEM((segs_here, 2 * bins_here), jnp.bfloat16),
            pltpu.VMEM((crowd, parts, segs_here, 2 * bins_here), jnp.bfloat16),
            pltpu.VMEM((RADIX, parts * halves, 2 * SUB, width), jnp.float32),
            pltpu.VMEM((parts // 2, LANES, 2 * LANES), jnp.bfloat16),
            pltpu.VMEM((RADIX, 2 * bins // RADIX, width), jnp.bfloat16),
            pltpu.VMEM((groups, RADIX, 2 * SUB, width), jnp.bfloat16),
            pltpu.VMEM((parts, tiles, 1, width), jnp.float32),
            dma((tiles,)), dma((4,)),
            dma((tiles, parts)), dma((tiles, parts)),
            dma((parts,)), dma((parts,)),
            dma((crowd,)), dma((crowd,)),
            dma((parts,)), dma((parts,)),
        ],
        compiler_params=pltpu.CompilerParams(
            vmem_limit_bytes=56 * 1024 * 1024, collective_id=0, has_side_effects=True
        ),
    )(templates, spectra.transpose(1, 2, 0), valid_start, jnp.asarray(base), jnp.asarray(turn), jnp.asarray(second))
    return out.T


def fits(spectra, templates):
    parts = lax.axis_size("freq")
    segs = spectra.shape[2] * lax.axis_size("group")
    bins_here, _, rows_here = templates.shape
    return (
        parts == SUB
        and rows_here % LANES == 0
        and bins_here % (SUB * RADIX) == 0
        and LANES // parts * segs == 2 * LANES
    )


def dispatch(spectra, templates, valid_start):
    if fits(spectra, templates):
        return fused(spectra, templates, valid_start)
    return on_device(spectra, templates, valid_start)


def solution(mesh):
    in_specs = (P("freq", None, "group"), P("freq", None, "group"), P())
    out_specs = P("group", None)
    return jax.shard_map(
        dispatch, mesh=mesh, in_specs=in_specs, out_specs=out_specs, check_vma=False
    )
```

```python
import functools
import math

import jax
import jax.numpy as jnp
import numpy as np
from jax import lax
from jax.experimental import pallas as pl
from jax.experimental.pallas import tpu as pltpu
from jax.sharding import PartitionSpec as P

LANES = 128
RADIX = 16
SUB = 8
SCALE = 1.1328125
AHEAD = 3


def rotation(angle, row_axis, col_axis):
    cosine, sine = np.cos(angle), np.sin(angle)
    top = np.stack([cosine, -sine], col_axis)
    bottom = np.stack([sine, cosine], col_axis)
    return np.stack([top, bottom], row_axis)


def tables(bins):
    lags = 2 * bins
    inner = lags // RADIX
    a = np.arange(bins // RADIX)
    tau1 = np.arange(inner)
    angle = 2.0 * math.pi * ((tau1[:, None] * a[None, :]) % inner) / inner
    first = rotation(angle.reshape(inner // SUB, SUB, a.size), 1, 2)
    first = first.reshape(inner // SUB, 2, SUB, 2 * a.size)
    turn = 2.0 * math.pi * tau1.reshape(inner // SUB, SUB, 1) / lags
    turn = np.stack([np.cos(turn), np.sin(turn)], 0)
    b = np.arange(RADIX)
    angle = 2.0 * math.pi * ((b[:, None] * b[None, :]) % RADIX) / RADIX
    second = rotation(angle, 0, 2) * SCALE
    second = second.reshape(2 * RADIX, 2 * RADIX)
    second = np.kron(second, np.eye(SUB))
    return first.astype(np.float32), turn.astype(np.float32), second.astype(jnp.bfloat16)


def kernel(valid, r_ref, d_ref, base_ref, turn_ref, w2_ref, vs_ref, out_ref, work_ref, w1_ref, dexp_ref, y_ref):
    step = pl.program_id(0)
    width = out_ref.shape[2]
    parts, _, depth2, _ = r_ref.shape
    depth = depth2 // 2
    segs = d_ref.shape[3]
    per_tile = LANES // segs
    half = parts * depth
    rows2, cols2 = w2_ref.shape
    groups = y_ref.shape[0]
    inner = groups * SUB

    @pl.when(step == 0)
    def _():
        work_ref[...] = base_ref[...]

        @pl.loop(0, RADIX)
        def _(b):
            w1_ref[b] = work_ref[...].reshape(w1_ref.shape[1:]).astype(jnp.bfloat16)
            top, bottom = work_ref[:, 0], work_ref[:, 1]
            cosine, sine = turn_ref[0], turn_ref[1]
            work_ref[:, 0] = top * cosine - bottom * sine
            work_ref[:, 1] = bottom * cosine + top * sine

        seg_spread = (
            lax.broadcasted_iota(jnp.int32, (segs, LANES), 0)
            == lax.broadcasted_iota(jnp.int32, (segs, LANES), 1) // per_tile
        ).astype(jnp.bfloat16)

        @pl.loop(0, RADIX)
        def _(b):
            piece = d_ref[:, b].reshape(2 * half, segs)
            dexp_ref[b] = jnp.dot(piece, seg_spread, preferred_element_type=jnp.float32)

    lane = lax.broadcasted_iota(jnp.int32, (LANES, width), 1)
    wanted = step * (width // segs) + (lane // LANES) * per_tile + lane % per_tile
    pick = (lax.broadcasted_iota(jnp.int32, (LANES, width), 0) == wanted).astype(jnp.bfloat16)

    def split(x):
        x = x.reshape(parts, 2, depth, x.shape[1])
        return x[:, 0].reshape(half, -1), x[:, 1].reshape(half, -1)

    def first_stage(b, norm):
        bank = jnp.dot(
            r_ref[:, b].reshape(2 * half, LANES), pick, preferred_element_type=jnp.float32
        )
        h0, h1 = split(bank)
        d0, d1 = split(dexp_ref[b])
        d0 = jnp.concatenate([d0] * (width // LANES), 1)
        d1 = jnp.concatenate([d1] * (width // LANES), 1)
        square = h0 * h0 + h1 * h1
        norm = norm + jnp.sum(square.reshape(half // SUB, SUB, width), 0)
        cross = jnp.concatenate([h0 * d0 + h1 * d1, h0 * d1 - h1 * d0], 0).astype(jnp.bfloat16)
        y = jnp.dot(w1_ref[b], cross, preferred_element_type=jnp.float32)
        y_ref[:, b] = y.astype(jnp.bfloat16).reshape(groups, 2 * SUB, width)
        return norm

    norm = lax.fori_loop(
        0, RADIX, first_stage, jnp.zeros((SUB, width), jnp.float32), unroll=2
    )
    offset = lax.broadcasted_iota(jnp.int32, (SUB, width), 0) - vs_ref[...]
    row = lax.broadcasted_iota(jnp.int32, (RADIX, SUB, width), 0) * inner

    def second_stage(g, best):
        z = jnp.dot(
            w2_ref[...], y_ref[g].reshape(cols2, width), preferred_element_type=jnp.float32
        )
        re, im = z[: rows2 // 2], z[rows2 // 2 :]
        power = (re * re + im * im).reshape(RADIX, SUB, width)
        late = row + (offset + g * SUB)[None]
        inside = (late >= 0) & (late < valid)
        return jnp.maximum(best, jnp.max(jnp.where(inside, power, 0.0), 0))

    best = lax.fori_loop(
        0, groups, second_stage, jnp.zeros((SUB, width), jnp.float32), unroll=4
    )
    norm = jnp.sum(norm, 0, keepdims=True) * (SCALE * SCALE)
    out_ref[0] = jnp.max(best, 0, keepdims=True) / norm


def correlate(received, strain, starts, rows):
    parts, _, depth2, _ = received.shape
    segs = strain.shape[3]
    bins = parts * RADIX * depth2 // 2
    base, turn, second = tables(bins)
    per_tile = LANES // segs
    tiles = -(-rows // per_tile)
    width = 2 * LANES if tiles % 2 == 0 else LANES
    steps = tiles * LANES // width
    starts = jnp.tile(jnp.repeat(starts, per_tile), width // LANES)
    starts = jnp.broadcast_to(starts[None, :], (SUB, width))
    groups = 2 * bins // RADIX // SUB
    whole = pl.BlockSpec(memory_space=pltpu.VMEM)
    out = pl.pallas_call(
        functools.partial(kernel, bins),
        grid=(steps,),
        out_shape=jax.ShapeDtypeStruct((steps, 1, width), jnp.float32),
        in_specs=[whole] * 6,
        out_specs=pl.BlockSpec((1, 1, width), lambda i: (i, 0, 0)),
        scratch_shapes=[
            pltpu.VMEM(base.shape, jnp.float32),
            pltpu.VMEM((RADIX, groups * 2 * SUB, 2 * bins // RADIX), jnp.bfloat16),
            pltpu.VMEM((RADIX, parts * depth2, LANES), jnp.float32),
            pltpu.VMEM((groups, RADIX, 2 * SUB, width), jnp.bfloat16),
        ],
        compiler_params=pltpu.CompilerParams(vmem_limit_bytes=50 * 1024 * 1024),
    )(received, strain, jnp.asarray(base), jnp.asarray(turn), jnp.asarray(second), starts)
    out = out.reshape(tiles, segs, per_tile)
    return out.transpose(0, 2, 1).reshape(tiles * per_tile, segs)[:rows]


def join_parts(pieces, depth):
    if depth % SUB == 0:
        return pieces
    parts, _, _, last = pieces.shape
    pieces = pieces.reshape(parts, RADIX, 2, depth, last).transpose(1, 2, 0, 3, 4)
    return pieces.reshape(1, RADIX, 2 * parts * depth, last)


def share(piece, axes):
    count = lax.axis_size(axes)
    return lax.all_to_all(jnp.broadcast_to(piece[None], (count,) + piece.shape), axes, 0, 0, tiled=True)


def on_device(spectra, templates, valid_start):
    parts = lax.axis_size("freq")
    bins_here, _, rows_here = templates.shape
    depth = bins_here // RADIX
    rows = rows_here // parts
    bank = templates.reshape(depth, RADIX, 2, parts, rows).transpose(3, 1, 2, 0, 4)
    strain = share(spectra.reshape(bins_here * 2, -1).T, "group")
    segs = strain.shape[0] * strain.shape[1]
    strain = strain.reshape(segs, depth, RADIX, 2).transpose(2, 3, 1, 0)
    strain = jnp.broadcast_to(strain[None], (parts,) + strain.shape)
    bank = jnp.concatenate([bank, strain], 4)
    bank = jnp.pad(bank, ((0, 0),) * 4 + ((0, LANES - rows - segs),))
    bank = bank.reshape(parts, RADIX, 2 * depth, LANES)
    received = lax.all_to_all(bank, "freq", 0, 0, tiled=True)
    strain = received[..., rows : rows + segs]
    peaks = correlate(join_parts(received, depth), join_parts(strain, depth), valid_start, rows)
    peaks = share(peaks.reshape(1, -1), "freq")
    return peaks.reshape(rows_here, -1)


MESH = pl.DeviceIdType.MESH


def fused_tables(bins):
    base, turn, _ = tables(bins)
    groups, _, _, cols = base.shape
    base = base.reshape(groups, 2, SUB, 2, cols // (2 * SUB), SUB)
    base = base.transpose(0, 1, 2, 4, 3, 5).reshape(groups, 2, SUB, cols)
    b = np.arange(RADIX)
    angle = 2.0 * math.pi * ((b[: RADIX * 3 // 4, None] * b[None, :]) % RADIX) / RADIX
    second = rotation(angle, 0, 2) * SCALE
    second = np.kron(second.reshape(-1, 2 * RADIX), np.eye(SUB))
    return base, turn, second.astype(jnp.bfloat16)


def block_transpose(rows, size):
    count = len(rows)
    lane = lax.broadcasted_iota(jnp.int32, rows[0].shape, rows[0].ndim - 1) // size
    step = count // 2
    while step:
        low = (lane // step) % 2 == 0
        fresh = list(rows)
        for i in range(count):
            if i & step == 0:
                first, second = rows[i], rows[i + step]
                axis = first.ndim - 1
                fresh[i] = jnp.where(low, first, pltpu.roll(second, size * step, axis))
                fresh[i + step] = jnp.where(low, pltpu.roll(first, LANES - size * step, axis), second)
        rows = fresh
        step //= 2
    return rows


def corner_turn(x, size):
    row = lax.broadcasted_iota(jnp.int32, x.shape, 0)
    block = lax.broadcasted_iota(jnp.int32, x.shape, 1) // size
    step = SUB // 2
    while step:
        low, left = (row // step) % 2, (block // step) % 2
        below = pltpu.roll(pltpu.roll(x, SUB - step, 0), size * step, 1)
        above = pltpu.roll(pltpu.roll(x, step, 0), LANES - size * step, 1)
        x = jnp.where(low == left, x, jnp.where(low == 0, below, above))
        step //= 2
    return x


def fused_kernel(
    x_hbm, s_hbm, vs_ref, base_hbm, turn_hbm, w2_hbm, out_ref,
    x_ref, own_ref, send_ref, recv_ref, work_ref, turn_ref, w2_ref, w1_ref, s_ref, strain_ref, dexp_ref,
    pick_ref, cross_ref, y_ref, peak_ref,
    load_sem, table_sem, send_sem, recv_sem, ssend_sem, srecv_sem, gsend_sem, grecv_sem, psend_sem, precv_sem,
):
    tiles, parts = recv_ref.shape[:2]
    halves, highs = recv_ref.shape[2:4]
    lows = RADIX // highs
    size = LANES // parts
    segs = vs_ref.shape[0]
    width = y_ref.shape[3]
    groups = y_ref.shape[0]
    crowd = strain_ref.shape[0]
    bins_here = x_ref.shape[1]
    rows = 2 * SUB * RADIX
    lags = 2 * parts * bins_here
    inner = lags // RADIX
    quarter = lags // 4
    blocks = parts * halves
    me = lax.axis_index("freq")
    team = lax.axis_index("group")

    def others(count, here):
        hops = sorted(range(1, count), key=lambda hop: (-min(hop, count - hop), hop))
        return [lax.rem(here + hop, count) for hop in hops]

    def load(tile):
        return pltpu.make_async_copy(
            x_hbm.at[:, :, pl.ds(tile * LANES, LANES)], x_ref.at[tile], load_sem.at[tile]
        )

    table_copies = [
        pltpu.make_async_copy(s_hbm, own_ref, table_sem.at[0]),
        pltpu.make_async_copy(base_hbm, work_ref, table_sem.at[1]),
        pltpu.make_async_copy(turn_hbm, turn_ref, table_sem.at[2]),
        pltpu.make_async_copy(w2_hbm, w2_ref, table_sem.at[3]),
    ]
    table_copies[0].start()
    for tile in range(tiles):
        load(tile).start()
    for copy in table_copies[1:]:
        copy.start()

    barrier = pltpu.get_barrier_semaphore()
    for target in others(parts, me):
        pl.semaphore_signal(barrier, inc=1, device_id={"freq": target}, device_id_type=MESH)
    for target in others(crowd, team):
        pl.semaphore_signal(barrier, inc=1, device_id={"group": target}, device_id_type=MESH)

    def strain_copy(source, target):
        return pltpu.make_async_remote_copy(
            src_ref=s_ref, dst_ref=strain_ref.at[team, source],
            send_sem=ssend_sem.at[target], recv_sem=srecv_sem.at[source],
            device_id={"freq": target}, device_id_type=MESH,
        )

    def team_copy(source, target):
        return pltpu.make_async_remote_copy(
            src_ref=strain_ref.at[team], dst_ref=strain_ref.at[source],
            send_sem=gsend_sem.at[target], recv_sem=grecv_sem.at[source],
            device_id={"group": target}, device_id_type=MESH,
        )

    def bank_copy(tile, source, target):
        return pltpu.make_async_remote_copy(
            src_ref=send_ref.at[tile, target], dst_ref=recv_ref.at[tile, source],
            send_sem=send_sem.at[tile, target], recv_sem=recv_sem.at[tile, source],
            device_id={"freq": target}, device_id_type=MESH,
        )

    def peak_copy(source, target):
        return pltpu.make_async_remote_copy(
            src_ref=peak_ref.at[me], dst_ref=peak_ref.at[source],
            send_sem=psend_sem.at[target], recv_sem=precv_sem.at[source],
            device_id={"freq": target}, device_id_type=MESH,
        )

    place = lax.broadcasted_iota(jnp.int32, (rows, rows), 0)
    origin = ((place % SUB) * RADIX + place // (2 * SUB)) * 2 + (place // SUB) % 2
    sort = (lax.broadcasted_iota(jnp.int32, (rows, rows), 1) == origin).astype(jnp.bfloat16)

    table_copies[0].wait()
    for tile in range(tiles):
        load(tile).wait()
    place = lax.broadcasted_iota(jnp.int32, (rows, rows), 1)
    origin = ((place // SUB) % 2 * SUB + place % SUB) * RADIX + place // (2 * SUB)
    order = (lax.broadcasted_iota(jnp.int32, (rows, rows), 0) == origin).astype(jnp.bfloat16)
    span = SUB * RADIX
    strain = []
    for h in range(halves):
        piece = jnp.concatenate([own_ref[c, :, h * span : (h + 1) * span] for c in range(2)], 1)
        strain.append(jnp.dot(piece, order, preferred_element_type=jnp.float32))
    strain = jnp.concatenate(strain, 1)
    lane = lax.broadcasted_iota(jnp.int32, strain.shape, 1)
    row = lax.broadcasted_iota(jnp.int32, strain.shape, 0)
    start = jnp.zeros(strain.shape, jnp.int32)
    for s in range(strain.shape[0]):
        start = jnp.where(row == s, vs_ref[team * strain.shape[0] + s], start)
    turns = (start >= quarter).astype(jnp.int32) + (start >= 2 * quarter).astype(jnp.int32)
    turns = (turns * (lane // (2 * SUB))) % 4
    imaginary = (lane // SUB) % 2 == 1
    wide = strain.shape[1]
    swapped = jnp.where(imaginary, pltpu.roll(strain, SUB, 1), -pltpu.roll(strain, wide - SUB, 1))
    strain = jnp.where(turns % 2 == 1, swapped, strain)
    s_ref[...] = jnp.where(turns >= 2, -strain, strain).astype(jnp.bfloat16)
    for tile in range(tiles):
        x = x_ref[tile].reshape(halves, rows, LANES)
        x = jnp.stack([jnp.dot(sort, x[h], preferred_element_type=jnp.float32) for h in range(halves)])
        x = x.reshape(halves * highs, lows, 2 * SUB, LANES)
        x = block_transpose([x[:, i] for i in range(lows)], size)
        for p in range(parts):
            send_ref[tile, p] = x[p].astype(jnp.bfloat16).reshape(halves, highs, 2 * SUB, LANES)

    pl.semaphore_wait(barrier, parts + crowd - 2)
    for target in others(parts, me):
        strain_copy(me, target).start()
    ahead = min(AHEAD, tiles)
    for target in others(parts, me):
        bank_copy(0, me, target).start()
    strain_ref[team, me] = s_ref[...]
    for tile in range(tiles):
        recv_ref[tile, me] = send_ref[tile, me]

    bank_row = lax.broadcasted_iota(jnp.int32, (LANES, 2 * LANES), 0)
    bank_lane = lax.broadcasted_iota(jnp.int32, (LANES, 2 * LANES), 1)
    for pair in range(lows // 2):
        wanted = (2 * pair + bank_lane // LANES) * size + bank_lane % size
        pick_ref[pair] = (bank_row == wanted).astype(jnp.bfloat16)
    collect = (bank_row % size == bank_lane % size).astype(jnp.float32)
    seg = lax.broadcasted_iota(jnp.int32, (SUB, width), 1) // size
    start = jnp.zeros((SUB, width), jnp.int32)
    for s in range(segs):
        start = jnp.where(seg == s, vs_ref[s], start)
    offset = lax.broadcasted_iota(jnp.int32, (SUB, width), 0) - start % quarter

    for copy in table_copies[1:]:
        copy.wait()

    @pl.loop(0, RADIX)
    def _(b):
        w1_ref[b] = work_ref[...].reshape(w1_ref.shape[1:]).astype(jnp.bfloat16)
        top, bottom = work_ref[:, 0], work_ref[:, 1]
        cosine, sine = turn_ref[0], turn_ref[1]
        work_ref[:, 0] = top * cosine - bottom * sine
        work_ref[:, 1] = bottom * cosine + top * sine

    for source in others(parts, me):
        strain_copy(source, source).wait_recv()
    for target in others(crowd, team):
        team_copy(team, target).start()
    for tile in range(1, ahead):
        for target in others(parts, me):
            bank_copy(tile, me, target).start()
    for source in others(crowd, team):
        team_copy(source, source).wait_recv()

    lane_seg = lax.broadcasted_iota(jnp.int32, (segs, width), 1) // size
    spread = (lax.broadcasted_iota(jnp.int32, (segs, width), 0) == lane_seg).astype(jnp.bfloat16)
    for f in range(parts):
        piece = jnp.concatenate([strain_ref[g, f] for g in range(crowd)], 0)
        piece = lax.dot_general(
            piece, spread, (((0,), (0,)), ((), ())), preferred_element_type=jnp.float32
        )
        piece = piece.reshape(halves, RADIX, 2 * SUB, width)
        for h in range(halves):
            dexp_ref[:, f * halves + h] = piece[h]

    def expand(tile, high, pair):
        piece = recv_ref[tile, :, :, high].reshape(blocks * 2 * SUB, LANES)
        bank = jnp.dot(piece, pick_ref[pair], preferred_element_type=jnp.float32)
        bank = bank.reshape(blocks, 2 * SUB, 2 * LANES)
        for k in range(2):
            b = high * lows + 2 * pair + k
            h0 = bank[:, :SUB, k * LANES : (k + 1) * LANES]
            h1 = bank[:, SUB:, k * LANES : (k + 1) * LANES]
            for side in range(width // LANES):
                here = slice(side * LANES, (side + 1) * LANES)
                d0, d1 = dexp_ref[b, :, :SUB, here], dexp_ref[b, :, SUB:, here]
                cross = jnp.concatenate([h0 * d0 + h1 * d1, h0 * d1 - h1 * d0], 1)
                cross_ref[b, :, here] = cross.reshape(blocks * 2 * SUB, LANES).astype(jnp.bfloat16)

    def transform(high, pair):
        for k in range(2):
            b = high * lows + 2 * pair + k
            y = jnp.dot(w1_ref[b], cross_ref[b], preferred_element_type=jnp.float32)
            y_ref[:, b] = y.astype(jnp.bfloat16).reshape(groups, 2 * SUB, width)

    def arrive(tile):
        for source in others(parts, me):
            bank_copy(tile, source, source).wait_recv()


    @pl.loop(0, tiles)
    def _(tile):
        arrive(tile)

        @pl.when(tile + ahead < tiles)
        def _():
            for target in others(parts, me):
                bank_copy(tile + ahead, me, target).start()

        pairs = [(high, pair) for high in range(highs) for pair in range(lows // 2)]
        expand(tile, *pairs[0])
        for now, later in zip(pairs, pairs[1:] + [None]):
            if later is not None:
                expand(tile, *later)
            transform(*now)

        def add_squares(f, total):
            piece = recv_ref[tile, f].astype(jnp.float32).reshape(-1, SUB, LANES)
            return total + jnp.sum(piece * piece, 0)

        norm = jnp.zeros((SUB, LANES), jnp.float32)
        for f in range(parts):
            norm = add_squares(f, norm)
        norm = jnp.dot(norm, collect, precision=lax.Precision.HIGHEST, preferred_element_type=jnp.float32)
        norm = jnp.sum(norm, 0, keepdims=True) * (SCALE * SCALE)

        def second_stage(g, best):
            z = jnp.dot(
                w2_ref[...], y_ref[g].reshape(w2_ref.shape[1], width), preferred_element_type=jnp.float32
            )
            z = z.reshape(2, -1, SUB, width)
            for t in range(RADIX // 2):
                re, im = z[0, t], z[1, t]
                if t + RADIX // 2 < z.shape[1]:
                    inside = offset >= -(g * SUB + t * inner)
                    re = jnp.where(inside, re, z[0, t + RADIX // 2])
                    im = jnp.where(inside, im, z[1, t + RADIX // 2])
                best = jnp.maximum(best, re * re + im * im)
            return best

        best = lax.fori_loop(
            0, groups, second_stage, jnp.zeros((SUB, width), jnp.float32), unroll=32
        )
        peak_ref[me, tile] = jnp.max(best, 0, keepdims=True) / norm

    for target in others(parts, me):
        peak_copy(me, target).start()
    for target in others(parts, me):
        strain_copy(me, target).wait_send()
        for tile in range(tiles):
            bank_copy(tile, me, target).wait_send()
    for target in others(crowd, team):
        team_copy(team, target).wait_send()
    for source in others(parts, me):
        peak_copy(source, source).wait_recv()
    for tile in range(tiles):
        peaks = jnp.concatenate([peak_ref[p, tile] for p in range(parts)], 0)
        for side in range(width // LANES):
            out_ref[side * SUB : (side + 1) * SUB, tile * LANES : (tile + 1) * LANES] = corner_turn(
                peaks[:, side * LANES : (side + 1) * LANES], size
            )
    for target in others(parts, me):
        peak_copy(me, target).wait_send()


def fused(spectra, templates, valid_start):
    parts, crowd = lax.axis_size("freq"), lax.axis_size("group")
    bins_here, _, rows_here = templates.shape
    segs_here = spectra.shape[2]
    segs = segs_here * crowd
    bins = bins_here * parts
    tiles = rows_here // LANES
    halves = bins_here // (SUB * RADIX)
    highs = RADIX // parts
    width = LANES // parts * segs
    base, turn, second = fused_tables(bins)
    groups = 2 * bins // RADIX // SUB
    far = pl.BlockSpec(memory_space=pltpu.HBM)
    whole = pl.BlockSpec(memory_space=pltpu.VMEM)
    dma = pltpu.SemaphoreType.DMA
    chunk = (halves, highs, 2 * SUB, LANES)
    out = pl.pallas_call(
        fused_kernel,
        out_shape=jax.ShapeDtypeStruct((segs, rows_here), jnp.float32),
        in_specs=[far, far, pl.BlockSpec(memory_space=pltpu.SMEM), far, far, far],
        out_specs=whole,
        scratch_shapes=[
            pltpu.VMEM((tiles, bins_here, 2, LANES), jnp.bfloat16),
            pltpu.VMEM((2, segs_here, bins_here), jnp.bfloat16),
            pltpu.VMEM((tiles, parts) + chunk, jnp.bfloat16),
            pltpu.VMEM((tiles, parts) + chunk, jnp.bfloat16),
            pltpu.VMEM(base.shape, jnp.float32),
            pltpu.VMEM(turn.shape, jnp.float32),
            pltpu.VMEM(second.shape, jnp.bfloat16),
            pltpu.VMEM((RADIX, groups * 2 * SUB, 2 * bins // RADIX), jnp.bfloat16),
            pltpu.VMEM((segs_here, 2 * bins_here), jnp.bfloat16),
            pltpu.VMEM((crowd, parts, segs_here, 2 * bins_here), jnp.bfloat16),
            pltpu.VMEM((RADIX, parts * halves, 2 * SUB, width), jnp.float32),
            pltpu.VMEM((parts // 2, LANES, 2 * LANES), jnp.bfloat16),
            pltpu.VMEM((RADIX, 2 * bins // RADIX, width), jnp.bfloat16),
            pltpu.VMEM((groups, RADIX, 2 * SUB, width), jnp.bfloat16),
            pltpu.VMEM((parts, tiles, 1, width), jnp.float32),
            dma((tiles,)), dma((4,)),
            dma((tiles, parts)), dma((tiles, parts)),
            dma((parts,)), dma((parts,)),
            dma((crowd,)), dma((crowd,)),
            dma((parts,)), dma((parts,)),
        ],
        compiler_params=pltpu.CompilerParams(
            vmem_limit_bytes=56 * 1024 * 1024, collective_id=0, has_side_effects=True
        ),
    )(templates, spectra.transpose(1, 2, 0), valid_start, jnp.asarray(base), jnp.asarray(turn), jnp.asarray(second))
    return out.T


def fits(spectra, templates):
    parts = lax.axis_size("freq")
    segs = spectra.shape[2] * lax.axis_size("group")
    bins_here, _, rows_here = templates.shape
    return (
        parts == SUB
        and rows_here % LANES == 0
        and bins_here % (SUB * RADIX) == 0
        and LANES // parts * segs == 2 * LANES
    )


def dispatch(spectra, templates, valid_start):
    if fits(spectra, templates):
        return fused(spectra, templates, valid_start)
    return on_device(spectra, templates, valid_start)


def solution(mesh):
    in_specs = (P("freq", None, "group"), P("freq", None, "group"), P())
    out_specs = P("group", None)
    return jax.shard_map(
        dispatch, mesh=mesh, in_specs=in_specs, out_specs=out_specs, check_vma=False
    )
```
